32 devices in a mesh: blk: 8 (over y, x, core), walk: 4 (over z).
Axes of the slice: x: 2, y: 2, z: 4, core: 2. Of those that a mesh axis runs over, the one named last changes fastest.
Arguments:
- walker_m: bfloat16 [4, 8, 128, 128], P('walk', 'blk'), may hold values from -6 to 6
- vertex_times: int32 [4, 8, 128], P('walk', 'blk'), may hold values from 0 to 1023
- vertex_labels: int32 [4, 8, 128], P('walk', 'blk'), may hold values from 0 to 35
- freq_index: int32 [24], replicated, may hold values from -64 to 63
- q_index: int32 [8], P('blk'), may hold values from 0 to 35
Outputs:
- g4: float32 [8, 2, 864, 864], P('blk', None, 'walk')
The draws below stay inside these ranges and needn't reach their ends.
Inputs may be any that keep to these rules, and one draw needn't show every extreme that they name: `q_index`: entry b is 6 qx + qy for the transfer momentum (qx, qy). `freq_index`: frequency f is pi (2 n + 1) / beta with n its entry. `vertex_times`: the time is entry * beta / 1024. `vertex_labels`: site s lies at row s // 6 and column s mod 6 of the 6×6 cluster.
All inputs are finite; a program needn't handle non-finite values.
Results may differ from the reference program's by a relative error of at most 0.0061.
Values may be sent and summed in bfloat16 or wider, within the bound.
A program may use at most 128 MiB of HBM per device.

```python
import math
import jax
import jax.numpy as jnp
from jax import lax

SIDE = 6
NK = 36
NF = 24
K = 864
V = 128
STEPS = 4
TGRID = 1024
OWNERS = 8
GROUPS = 4
N_BLK = 8
N_WALK = 4


def touch_ends(drawn, key, low, high):
    dims = drawn.shape
    place = [jax.random.randint(jax.random.fold_in(key, axis), (), 0, dims[axis]) for axis in range(len(dims))]
    drawn = drawn.at[tuple(place)].set(low)
    longest = dims.index(max(dims))
    place[longest] = (place[longest] + 1) % dims[longest]
    return drawn.at[tuple(place)].set(high)


def block_levels(stream_key, dims, cuts, least, top_value):
    def one(dim, blocks):
        draws = jax.random.uniform(jax.random.fold_in(jax.random.fold_in(stream_key, 6), dim), (blocks,), jnp.float32, least / len(cuts), top_value / len(cuts))
        return jnp.repeat(jnp.exp(draws), dims[dim] // blocks).reshape((-1,) + (1,) * (len(dims) - dim - 1))

    factor_of = one(*cuts[0])
    for cut in cuts[1:]:
        factor_of = factor_of * one(*cut)
    return factor_of


def gaussian(stream_key, dims, width, reach, cuts=(), kind=jnp.bfloat16):
    loudness = block_levels(stream_key, dims, cuts, -0.22, 0.18) if cuts else 1.0
    values = jax.random.normal(stream_key, dims, jnp.float32) * width * loudness
    return jnp.minimum(jnp.maximum(values, -reach), reach).astype(kind)


def setup_inputs(seed: int = 0) -> dict:
    streams_of = jax.random.split(jax.random.key(seed), 6)
    return {
        "walker_m": gaussian(streams_of[0], (GROUPS, OWNERS, V, V), 1.0, 6.0, ((0, 4), (1, 8))),
        "vertex_times": touch_ends(jax.random.randint(streams_of[1], (GROUPS, OWNERS, V), 0, TGRID), jax.random.fold_in(streams_of[1], 1), 0, TGRID - 1).astype(jnp.int32),
        "vertex_labels": touch_ends(jax.random.randint(streams_of[2], (GROUPS, OWNERS, V), 0, NK), jax.random.fold_in(streams_of[2], 1), 0, NK - 1).astype(jnp.int32),
        "freq_index": touch_ends(jax.random.randint(streams_of[3], (NF,), -64, 64), jax.random.fold_in(streams_of[3], 1), -64, 63).astype(jnp.int32),
        "q_index": touch_ends(jax.random.randint(streams_of[4], (OWNERS,), 0, NK), jax.random.fold_in(streams_of[4], 1), 0, NK - 1).astype(jnp.int32),
    }


TWO_PI = 2.0 * math.pi


def phase_tables(time_points, labels, frequencies):
    modulus = 12 * TGRID
    momenta = jnp.arange(NK, dtype=jnp.int32)
    momentum_across = momenta // SIDE
    momentum_down = momenta % SIDE
    site_across = labels // SIDE
    site_down = labels % SIDE
    freq_part = jnp.mod((2 * frequencies[:, None] + 1) * time_points[None, :] * 6, modulus)
    momentum_part = jnp.mod(2 * TGRID * (momentum_across[:, None] * site_across[None, :] + momentum_down[:, None] * site_down[None, :]), modulus)
    phase = jnp.mod(freq_part[None, :, :] - momentum_part[:, None, :], modulus).reshape(NK * NF, -1)
    angles = phase.astype(jnp.float32) * (TWO_PI / modulus)
    return jnp.cos(angles).astype(jnp.bfloat16), jnp.sin(angles).astype(jnp.bfloat16)


def build_green(matrix, time_points, labels, frequencies):
    cos_table, sin_table = phase_tables(time_points, labels, frequencies)
    stacked = jnp.concatenate([cos_table, sin_table], axis=0)
    amplitude = jnp.dot(stacked, matrix, preferred_element_type=jnp.float32).astype(jnp.bfloat16)
    real_part = amplitude[:K]
    imag_part = amplitude[K:]
    left_side = jnp.concatenate([jnp.concatenate([real_part, imag_part], axis=1), jnp.concatenate([imag_part, -real_part], axis=1)], axis=0)
    right_side = jnp.concatenate([cos_table, sin_table], axis=1)
    green_table = lax.dot_general(left_side, right_side, (((1,), (1,)), ((), ())), preferred_element_type=jnp.float32)
    return (green_table * (1.0 / V)).reshape(2, K, K)


def shifted_rows(transfer):
    transfer = transfer.astype(jnp.int32)
    row_index = jnp.arange(K, dtype=jnp.int32)
    momentum = row_index // NF
    offset = row_index % NF
    shift_across = (momentum // SIDE + transfer // SIDE) % SIDE
    shift_down = (momentum % SIDE + transfer % SIDE) % SIDE
    return ((shift_across * SIDE + shift_down) * NF + offset).astype(jnp.int32)


def contribution(green_table, shifted):
    shifted_green = jnp.take(jnp.take(green_table, shifted, axis=1), shifted, axis=2)
    flipped = jnp.swapaxes(green_table, 1, 2)
    real_term = shifted_green[0] * flipped[0] - shifted_green[1] * flipped[1]
    imag_term = shifted_green[0] * flipped[1] + shifted_green[1] * flipped[0]
    return jnp.stack([real_term, imag_term])


def reference(walker_m, vertex_times, vertex_labels, freq_index, q_index):
    walker_count = N_WALK * N_BLK
    matrices = walker_m.reshape(walker_count, V, V)
    time_rows = vertex_times.reshape(walker_count, V)
    label_rows = vertex_labels.reshape(walker_count, V)
    sources = jnp.arange(walker_count, dtype=jnp.int32) % N_BLK

    def visit_walker(running, walker_item):
        matrix, time_points, labels, source = walker_item
        green_table = build_green(matrix, time_points, labels, freq_index)
        for number in range(STEPS):
            offset = number - (STEPS // 2 - 1)
            owner_index = jnp.mod(source - offset, N_BLK).astype(jnp.int32)
            addition = contribution(green_table, shifted_rows(q_index[owner_index]))
            running = running.at[owner_index].add(addition)
        return running, None

    start = jnp.zeros((N_BLK, 2, K, K), jnp.float32)
    running, unused = lax.scan(visit_walker, start, (matrices, time_rows, label_rows, sources))
    return running * (1.0 / (STEPS * N_WALK))
```

```python
import functools
import math

import jax
import jax.numpy as jnp
from jax import lax
from jax.experimental import pallas as pl
from jax.experimental.pallas import tpu as pltpu
from jax.sharding import PartitionSpec as P

SIDE = 6
TGRID = 1024
OFFSETS = (0, 1, -1, 2)
FORWARD = (2, 3, 4)


def sine(units):
    wrapped = ((units + 1024) & 2047) - 1024
    folded = jnp.where(wrapped > 512, 1024 - wrapped, wrapped)
    folded = jnp.where(wrapped < -512, -1024 - wrapped, folded)
    x = folded.astype(jnp.float32) * (math.pi / 1024.0)
    y = x * x
    total = jnp.full_like(y, 1.0 / math.factorial(13))
    for order in (11, 9, 7, 5, 3, 1):
        sign = -1.0 if (order // 2) % 2 else 1.0
        total = total * y + sign / math.factorial(order)
    return total * x


def sixth_turn(m):
    r = m - 6 * ((m * 10923) >> 16)
    half = jnp.where((r == 1) | (r == 5), 0.5, -0.5)
    cosine = jnp.where(r == 0, 1.0, jnp.where(r == 3, -1.0, half))
    root = math.sqrt(3.0) / 2.0
    side = jnp.where(r < 3, root, -root)
    return cosine.astype(jnp.float32), jnp.where((r == 0) | (r == 3), 0.0, side).astype(jnp.float32)


def visits(groups):
    around = sorted(range(1, groups), key=lambda z: min(z, groups - z))
    near = [(0, d) for d in range(len(OFFSETS))]
    far = [(z, 0) for z in around]
    return near + far + [(z, d) for z in around for d in range(1, len(OFFSETS))]


def kernel(
    groups, owners, m_in, t_in, l_in, freq_ref, q_ref, out_ref,
    m_ref, t_ref, l_ref, send_sem, recv_sem,
    odd, plain, turned_m, table, lifted, left_s, left_f,
):
    order = visits(groups)
    walkers = len(order)
    w = lax.axis_index("walk")
    b = lax.axis_index("blk")

    def to_walk(z):
        return {"walk": lax.rem(w + groups - z, groups)}

    def to_blk(d):
        return {"blk": lax.rem(b + owners - OFFSETS[d], owners)}

    def copies(sources, slot, device):
        return [
            pltpu.make_async_remote_copy(
                src_ref=source,
                dst_ref=held.at[slot],
                send_sem=send_sem.at[kind, slot],
                recv_sem=recv_sem.at[kind, slot],
                device_id=device,
                device_id_type=pl.DeviceIdType.MESH,
            )
            for kind, (source, held) in enumerate(zip(sources, (m_ref, t_ref, l_ref)))
        ]

    own = (m_in.at[0, 0], t_in.at[0], l_in.at[0])

    def held_at(slot):
        return (m_ref.at[slot], t_ref.at[slot], l_ref.at[slot])

    def arrived(slot):
        for copy in copies(held_at(slot), slot, to_walk(1)):
            copy.wait_recv()

    barrier = pltpu.get_barrier_semaphore()
    peers = [{"walk": lax.rem(w + z, groups)} for z in range(1, groups)]
    reach = sorted({d % owners for d in OFFSETS + tuple(-d for d in OFFSETS)} - {0})
    peers += [{"blk": lax.rem(b + d, owners)} for d in reach]
    for peer in peers:
        pl.semaphore_signal(barrier, inc=1, device_id=peer, device_id_type=pl.DeviceIdType.MESH)
    m_ref[0] = m_in[0, 0]
    t_ref[0] = t_in[0]
    l_ref[0] = l_in[0]
    plain[...] = jnp.zeros_like(plain)
    out_ref[...] = jnp.zeros_like(out_ref)
    pl.semaphore_wait(barrier, len(peers))
    for z, d in [o for o in order if o[0] and not o[1]] + [o for o in order if o[1] and not o[0]]:
        for copy in copies(own, order.index((z, d)), to_walk(z) if z else to_blk(d)):
            copy.start()

    def forward(z):
        slot = order.index((z, 0))
        arrived(slot)
        for d in range(1, len(OFFSETS)):
            for copy in copies(held_at(slot), order.index((z, d)), to_blk(d)):
                copy.start()


    nf = freq_ref.shape[0]
    v = m_ref.shape[-1]
    own = out_ref.shape[2]
    cols = out_ref.shape[3]
    window = lifted.shape[0]
    first = w * own
    spare = lax.rem(first, 16)
    start = pl.multiple_of(first - spare, 16)
    spare = pl.multiple_of(spare, 8)

    row = lax.broadcasted_iota(jnp.int32, (nf, v), 0)
    freq = jnp.zeros((nf, v), jnp.int32)
    for f in range(nf):
        freq = jnp.where(row == f, 2 * freq_ref[f] + 1, freq)
    odd[...] = freq
    q = q_ref[0]
    qx = (q * 43) >> 8
    qy = q - SIDE * qx

    scale = 1.0 / (v * v * walkers)
    half = SIDE // 2
    low, high = slice(0, v), slice(v, 2 * v)
    contract = (((1,), (1,)), ((), ()))

    def sites(slot):
        labels = l_ref[slot]
        sx = (labels * 43) >> 8
        return sx, labels - SIDE * sx

    def build_table(slot):
        sx, sy = sites(slot)
        units = (odd[...] * t_ref[slot]) & 2047
        cx, ox = sixth_turn(sx)
        cy, oy = sixth_turn(sy)
        flip_x = (1 - 2 * (sx & 1)).astype(jnp.float32).astype(jnp.bfloat16)
        flip_y = (1 - 2 * (sy & 1)).astype(jnp.float32)
        c, s = sine(units + 512), sine(units)
        for kx in range(half):
            line = [(c, s)]
            for ky in range(1, half):
                c1, s1 = line[-1]
                line.append((c1 * cy + s1 * oy, s1 * cy - c1 * oy))
            line += [(c1 * flip_y, s1 * flip_y) for c1, s1 in line]
            for pair in range(half):
                rows = slice(nf * (SIDE * kx + 2 * pair), nf * (SIDE * kx + 2 * pair + 2))
                far = slice(rows.start + nf * SIDE * half, rows.stop + nf * SIDE * half)
                for side, lanes in enumerate((low, high)):
                    both = jnp.concatenate(
                        [line[2 * pair][side], line[2 * pair + 1][side]], axis=0
                    ).astype(jnp.bfloat16)
                    table[rows, lanes] = both
                    table[far, lanes] = both * flip_x
            c, s = c * cx + s * ox, s * cx - c * ox

    def place_m(slot):
        matrix = m_ref[slot]
        plain[low, low] = matrix
        plain[high, high] = matrix
        sx, sy = sites(slot)
        cu, su = sixth_turn(qx * sx + qy * sy)
        cu = jnp.broadcast_to(cu, (v, v))
        su = jnp.broadcast_to(su, (v, v))
        ct, st = cu.T, su.T
        wide = matrix.astype(jnp.float32) * scale
        re = (wide * (ct * cu + st * su)).astype(jnp.bfloat16)
        im = (wide * (ct * su - st * cu)).astype(jnp.bfloat16)
        turned_m[low, low] = re
        turned_m[high, high] = re
        turned_m[low, high] = im
        turned_m[high, low] = -im

    def lift():
        mine = table[pl.ds(start, window), :]
        lifted[:, 0 : 2 * v] = jnp.dot(mine, turned_m[...], preferred_element_type=jnp.float32)
        lifted[:, 2 * v : 4 * v] = lax.dot_general(
            mine, plain[...], contract, preferred_element_type=jnp.float32
        )
        for ref, base in ((left_s, 0), (left_f, 2 * v)):
            re = lifted[pl.ds(spare, own), base : base + v]
            im = lifted[pl.ds(spare, own), base + v : base + 2 * v]
            ref[:, low] = jnp.concatenate([re, im], axis=0).astype(jnp.bfloat16)
            ref[:, high] = jnp.concatenate([im, -re], axis=0).astype(jnp.bfloat16)

    def gather_terms():
        for begin in range(0, cols, 256):
            end = min(begin + 256, cols)
            shifted = lax.dot_general(
                left_s[...], table[begin:end], contract, preferred_element_type=jnp.float32
            )
            flipped = lax.dot_general(
                left_f[...], table[begin:end], contract, preferred_element_type=jnp.float32
            )
            sr, si = shifted[:own], shifted[own:]
            fr, fi = flipped[:own], flipped[own:]
            out_ref[0, 0, :, begin:end] += sr * fr + si * fi
            out_ref[0, 1, :, begin:end] += si * fr - sr * fi

    def step(visit, carry):
        swap = (lax.rem(b, 2) == 1) & ((visit == 1) | (visit == 2))
        i = jnp.where(swap, 3 - visit, visit)
        for turn, z in enumerate([z for z, d in order if z and not d]):
            @pl.when(visit == FORWARD[min(turn, len(FORWARD) - 1)])
            def _(z=z):
                forward(z)

        first_far = order.index((0, len(OFFSETS) - 1)) + 1
        last_far = first_far + groups - 1

        @pl.when(((visit > 0) & (visit < first_far)) | (visit >= last_far))
        def _():
            arrived(i)

        build_table(i)
        place_m(i)
        lift()
        gather_terms()
        return carry

    lax.fori_loop(0, walkers, step, 0)
    for slot in range(1, walkers):
        for copy in copies(held_at(slot), slot, to_walk(1)):
            copy.wait_send()


def local(walker_m, vertex_times, vertex_labels, freq_index, q_index):
    groups = lax.axis_size("walk")
    owners = lax.axis_size("blk")
    v = walker_m.shape[-1]
    nf = freq_index.shape[0]
    k = SIDE * SIDE * nf
    own = k // groups
    walkers = groups * len(OFFSETS)
    window = own if own % 16 == 0 else (own + 23) // 16 * 16
    held = max(k, max(own * w // 16 * 16 + window for w in range(groups)))
    vmem = pl.BlockSpec(memory_space=pltpu.VMEM)
    smem = pl.BlockSpec(memory_space=pltpu.SMEM)
    bf16 = jnp.bfloat16
    return pl.pallas_call(
        functools.partial(kernel, groups, owners),
        out_shape=pltpu.VMEM((1, 2, own, k), jnp.float32),
        in_specs=[vmem, vmem, vmem, smem, smem],
        out_specs=vmem,
        scratch_shapes=[
            pltpu.VMEM((walkers, v, v), bf16),
            pltpu.VMEM((walkers, 1, v), jnp.int32),
            pltpu.VMEM((walkers, 1, v), jnp.int32),
            pltpu.SemaphoreType.DMA((3, walkers)),
            pltpu.SemaphoreType.DMA((3, walkers)),
            pltpu.VMEM((nf, v), jnp.int32),
            pltpu.VMEM((2 * v, 2 * v), bf16),
            pltpu.VMEM((2 * v, 2 * v), bf16),
            pltpu.VMEM((held, 2 * v), bf16),
            pltpu.VMEM((window, 4 * v), jnp.float32),
            pltpu.VMEM((2 * own, 2 * v), bf16),
            pltpu.VMEM((2 * own, 2 * v), bf16),
        ],
        compiler_params=pltpu.CompilerParams(collective_id=0, has_side_effects=True),
    )(walker_m, vertex_times, vertex_labels, freq_index, q_index)


def solution(mesh):
    return jax.shard_map(
        local,
        mesh=mesh,
        in_specs=(
            P("walk", "blk", None, None),
            P("walk", "blk", None),
            P("walk", "blk", None),
            P(),
            P("blk"),
        ),
        out_specs=P("blk", None, "walk", None),
        check_vma=False,
    )
```

```python
import functools
import math

import jax
import jax.numpy as jnp
from jax import lax
from jax.experimental import pallas as pl
from jax.experimental.pallas import tpu as pltpu
from jax.sharding import PartitionSpec as P

SIDE = 6
TGRID = 1024
OFFSETS = (0, 1, -1, 2)
FORWARD = (2, 3, 4)


def sine(units):
    wrapped = ((units + 1024) & 2047) - 1024
    folded = jnp.where(wrapped > 512, 1024 - wrapped, wrapped)
    folded = jnp.where(wrapped < -512, -1024 - wrapped, folded)
    x = folded.astype(jnp.float32) * (math.pi / 1024.0)
    y = x * x
    total = jnp.full_like(y, 1.0 / math.factorial(13))
    for order in (11, 9, 7, 5, 3, 1):
        sign = -1.0 if (order // 2) % 2 else 1.0
        total = total * y + sign / math.factorial(order)
    return total * x


def sixth_turn(m):
    r = m - 6 * ((m * 10923) >> 16)
    half = jnp.where((r == 1) | (r == 5), 0.5, -0.5)
    cosine = jnp.where(r == 0, 1.0, jnp.where(r == 3, -1.0, half))
    root = math.sqrt(3.0) / 2.0
    side = jnp.where(r < 3, root, -root)
    return cosine.astype(jnp.float32), jnp.where((r == 0) | (r == 3), 0.0, side).astype(jnp.float32)


def visits(groups):
    around = sorted(range(1, groups), key=lambda z: min(z, groups - z))
    near = [(0, d) for d in range(len(OFFSETS))]
    far = [(z, 0) for z in around]
    return near + far + [(z, d) for z in around for d in range(1, len(OFFSETS))]


def kernel(
    groups, owners, m_in, t_in, l_in, freq_ref, q_ref, out_ref,
    m_ref, t_ref, l_ref, send_sem, recv_sem,
    odd, plain, turned_m, table, left_s, left_f,
):
    order = visits(groups)
    walkers = len(order)
    w = lax.axis_index("walk")
    b = lax.axis_index("blk")

    def to_walk(z):
        return {"walk": lax.rem(w + groups - z, groups)}

    def to_blk(d):
        return {"blk": lax.rem(b + owners - OFFSETS[d], owners)}

    def copies(sources, slot, device):
        return [
            pltpu.make_async_remote_copy(
                src_ref=source,
                dst_ref=held.at[slot],
                send_sem=send_sem.at[kind, slot],
                recv_sem=recv_sem.at[kind, slot],
                device_id=device,
                device_id_type=pl.DeviceIdType.MESH,
            )
            for kind, (source, held) in enumerate(zip(sources, (m_ref, t_ref, l_ref)))
        ]

    own = (m_in.at[0, 0], t_in.at[0], l_in.at[0])

    def held_at(slot):
        return (m_ref.at[slot], t_ref.at[slot], l_ref.at[slot])

    def arrived(slot):
        for copy in copies(held_at(slot), slot, to_walk(1)):
            copy.wait_recv()

    barrier = pltpu.get_barrier_semaphore()
    peers = [{"walk": lax.rem(w + z, groups)} for z in range(1, groups)]
    reach = sorted({d % owners for d in OFFSETS + tuple(-d for d in OFFSETS)} - {0})
    peers += [{"blk": lax.rem(b + d, owners)} for d in reach]
    for peer in peers:
        pl.semaphore_signal(barrier, inc=1, device_id=peer, device_id_type=pl.DeviceIdType.MESH)
    m_ref[0] = m_in[0, 0]
    t_ref[0] = t_in[0]
    l_ref[0] = l_in[0]
    plain[...] = jnp.zeros_like(plain)
    out_ref[...] = jnp.zeros_like(out_ref)
    pl.semaphore_wait(barrier, len(peers))
    for z, d in [o for o in order if o[0] and not o[1]] + [o for o in order if o[1] and not o[0]]:
        for copy in copies(own, order.index((z, d)), to_walk(z) if z else to_blk(d)):
            copy.start()

    def forward(z):
        slot = order.index((z, 0))
        arrived(slot)
        for d in range(1, len(OFFSETS)):
            for copy in copies(held_at(slot), order.index((z, d)), to_blk(d)):
                copy.start()


    nf = freq_ref.shape[0]
    v = m_ref.shape[-1]
    own = out_ref.shape[2]
    cols = out_ref.shape[3]
    window = own if own % 16 == 0 else (own + 23) // 16 * 16
    first = w * own
    spare = lax.rem(first, 16)
    start = pl.multiple_of(first - spare, 16)

    row = lax.broadcasted_iota(jnp.int32, (nf, v), 0)
    freq = jnp.zeros((nf, v), jnp.int32)
    for f in range(nf):
        freq = jnp.where(row == f, 2 * freq_ref[f] + 1, freq)
    odd[...] = freq
    q = q_ref[0]
    qx = (q * 43) >> 8
    qy = q - SIDE * qx

    scale = 1.0 / (v * v * walkers)
    half = SIDE // 2
    low, high = slice(0, v), slice(v, 2 * v)
    contract = (((1,), (1,)), ((), ()))

    def sites(slot):
        labels = l_ref[slot]
        sx = (labels * 43) >> 8
        return sx, labels - SIDE * sx

    def build_table(slot):
        sx, sy = sites(slot)
        units = (odd[...] * t_ref[slot]) & 2047
        cx, ox = sixth_turn(sx)
        cy, oy = sixth_turn(sy)
        flip_x = (1 - 2 * (sx & 1)).astype(jnp.float32).astype(jnp.bfloat16)
        flip_y = (1 - 2 * (sy & 1)).astype(jnp.float32)
        c, s = sine(units + 512), sine(units)
        for kx in range(half):
            line = [(c, s)]
            for ky in range(1, half):
                c1, s1 = line[-1]
                line.append((c1 * cy + s1 * oy, s1 * cy - c1 * oy))
            line += [(c1 * flip_y, s1 * flip_y) for c1, s1 in line]
            for pair in range(half):
                rows = slice(nf * (SIDE * kx + 2 * pair), nf * (SIDE * kx + 2 * pair + 2))
                far = slice(rows.start + nf * SIDE * half, rows.stop + nf * SIDE * half)
                for side, lanes in enumerate((low, high)):
                    both = jnp.concatenate(
                        [line[2 * pair][side], line[2 * pair + 1][side]], axis=0
                    ).astype(jnp.bfloat16)
                    table[rows, lanes] = both
                    table[far, lanes] = both * flip_x
            c, s = c * cx + s * ox, s * cx - c * ox

    def place_m(slot):
        matrix = m_ref[slot]
        plain[low, low] = matrix
        plain[high, high] = matrix
        sx, sy = sites(slot)
        cu, su = sixth_turn(qx * sx + qy * sy)
        cu = jnp.broadcast_to(cu, (v, v))
        su = jnp.broadcast_to(su, (v, v))
        ct, st = cu.T, su.T
        wide = matrix.astype(jnp.float32) * scale
        re = (wide * (ct * cu + st * su)).astype(jnp.bfloat16)
        im = (wide * (ct * su - st * cu)).astype(jnp.bfloat16)
        turned_m[low, low] = re
        turned_m[high, high] = re
        turned_m[low, high] = im
        turned_m[high, low] = -im

    def lift():
        mine = table[pl.ds(start, window), :]
        for ref, wide in (
            (left_s, jnp.dot(mine, turned_m[...], preferred_element_type=jnp.float32)),
            (left_f, lax.dot_general(mine, plain[...], contract, preferred_element_type=jnp.float32)),
        ):
            if window > own:
                wide = jnp.where(spare > 0, wide[8 : 8 + own], wide[:own])
            for tile in range(own // 8):
                part = wide[8 * tile : 8 * tile + 8]
                re, im = part[:, low], part[:, high]
                rows = slice(16 * tile, 16 * tile + 16)
                ref[rows, low] = jnp.concatenate([re, im], axis=0).astype(jnp.bfloat16)
                ref[rows, high] = jnp.concatenate([im, -re], axis=0).astype(jnp.bfloat16)

    def gather_terms():
        for begin in range(0, cols, 256):
            end = min(begin + 256, cols)
            shifted = lax.dot_general(
                left_s[...], table[begin:end], contract, preferred_element_type=jnp.float32
            )
            flipped = lax.dot_general(
                left_f[...], table[begin:end], contract, preferred_element_type=jnp.float32
            )
            for tile in range(own // 8):
                re, im = slice(16 * tile, 16 * tile + 8), slice(16 * tile + 8, 16 * tile + 16)
                rows = slice(8 * tile, 8 * tile + 8)
                sr, si, fr, fi = shifted[re], shifted[im], flipped[re], flipped[im]
                out_ref[0, 0, rows, begin:end] += sr * fr + si * fi
                out_ref[0, 1, rows, begin:end] += si * fr - sr * fi

    def step(visit, carry):
        swap = (lax.rem(b, 2) == 1) & ((visit == 1) | (visit == 2))
        i = jnp.where(swap, 3 - visit, visit)
        for turn, z in enumerate([z for z, d in order if z and not d]):
            @pl.when(visit == FORWARD[min(turn, len(FORWARD) - 1)])
            def _(z=z):
                forward(z)

        first_far = order.index((0, len(OFFSETS) - 1)) + 1
        last_far = first_far + groups - 1

        @pl.when(((visit > 0) & (visit < first_far)) | (visit >= last_far))
        def _():
            arrived(i)

        build_table(i)
        place_m(i)
        lift()
        gather_terms()
        return carry

    lax.fori_loop(0, walkers, step, 0)
    for slot in range(1, walkers):
        for copy in copies(held_at(slot), slot, to_walk(1)):
            copy.wait_send()


def local(walker_m, vertex_times, vertex_labels, freq_index, q_index):
    groups = lax.axis_size("walk")
    owners = lax.axis_size("blk")
    v = walker_m.shape[-1]
    nf = freq_index.shape[0]
    k = SIDE * SIDE * nf
    own = k // groups
    walkers = groups * len(OFFSETS)
    window = own if own % 16 == 0 else (own + 23) // 16 * 16
    held = max(k, max(own * w // 16 * 16 + window for w in range(groups)))
    vmem = pl.BlockSpec(memory_space=pltpu.VMEM)
    smem = pl.BlockSpec(memory_space=pltpu.SMEM)
    bf16 = jnp.bfloat16
    return pl.pallas_call(
        functools.partial(kernel, groups, owners),
        out_shape=pltpu.VMEM((1, 2, own, k), jnp.float32),
        in_specs=[vmem, vmem, vmem, smem, smem],
        out_specs=vmem,
        scratch_shapes=[
            pltpu.VMEM((walkers, v, v), bf16),
            pltpu.VMEM((walkers, 1, v), jnp.int32),
            pltpu.VMEM((walkers, 1, v), jnp.int32),
            pltpu.SemaphoreType.DMA((3, walkers)),
            pltpu.SemaphoreType.DMA((3, walkers)),
            pltpu.VMEM((nf, v), jnp.int32),
            pltpu.VMEM((2 * v, 2 * v), bf16),
            pltpu.VMEM((2 * v, 2 * v), bf16),
            pltpu.VMEM((held, 2 * v), bf16),
            pltpu.VMEM((2 * own, 2 * v), bf16),
            pltpu.VMEM((2 * own, 2 * v), bf16),
        ],
        compiler_params=pltpu.CompilerParams(collective_id=0, has_side_effects=True),
    )(walker_m, vertex_times, vertex_labels, freq_index, q_index)


def solution(mesh):
    return jax.shard_map(
        local,
        mesh=mesh,
        in_specs=(
            P("walk", "blk", None, None),
            P("walk", "blk", None),
            P("walk", "blk", None),
            P(),
            P("blk"),
        ),
        out_specs=P("blk", None, "walk", None),
        check_vma=False,
    )
```

```python
import functools
import math

import jax
import jax.numpy as jnp
from jax import lax
from jax.experimental import pallas as pl
from jax.experimental.pallas import tpu as pltpu
from jax.sharding import PartitionSpec as P

SIDE = 6
TGRID = 1024
OFFSETS = (0, 1, -1, 2)


def sine(units):
    wrapped = ((units + 1024) & 2047) - 1024
    folded = jnp.where(wrapped > 512, 1024 - wrapped, wrapped)
    folded = jnp.where(wrapped < -512, -1024 - wrapped, folded)
    x = folded.astype(jnp.float32) * (math.pi / 1024.0)
    y = x * x
    total = jnp.full_like(y, 1.0 / math.factorial(13))
    for order in (11, 9, 7, 5, 3, 1):
        sign = -1.0 if (order // 2) % 2 else 1.0
        total = total * y + sign / math.factorial(order)
    return total * x


def sixth_turn(m):
    r = m - 6 * ((m * 10923) >> 16)
    half = jnp.where((r == 1) | (r == 5), 0.5, -0.5)
    cosine = jnp.where(r == 0, 1.0, jnp.where(r == 3, -1.0, half))
    root = math.sqrt(3.0) / 2.0
    side = jnp.where(r < 3, root, -root)
    return cosine.astype(jnp.float32), jnp.where((r == 0) | (r == 3), 0.0, side).astype(jnp.float32)


def visits(groups):
    around = sorted(range(1, groups), key=lambda z: min(z, groups - z))
    near = [(0, d) for d in range(len(OFFSETS))]
    far = [(z, 0) for z in around]
    return near + far + [(z, d) for z in around for d in range(1, len(OFFSETS))]


def kernel(
    groups, owners, m_in, t_in, l_in, freq_ref, q_ref, out_ref,
    pack_ref, send_sem, recv_sem, odd, *stages,
):
    order = visits(groups)
    walkers = len(order)
    w = lax.axis_index("walk")
    b = lax.axis_index("blk")
    v = m_in.shape[-1]
    nf = freq_ref.shape[0]
    own = out_ref.shape[2]
    cols = out_ref.shape[3]
    even, odds = stages[: len(stages) // 2], stages[len(stages) // 2 :]

    def to_walk(z):
        return {"walk": lax.rem(w + groups - z, groups)}

    def to_blk(d):
        return {"blk": lax.rem(b + owners - OFFSETS[d], owners)}

    def copy(source, slot, device):
        return pltpu.make_async_remote_copy(
            src_ref=pack_ref.at[source],
            dst_ref=pack_ref.at[slot],
            send_sem=send_sem.at[slot],
            recv_sem=recv_sem.at[slot],
            device_id=device,
            device_id_type=pl.DeviceIdType.MESH,
        )

    def arrived(slot):
        copy(0, slot, to_walk(1)).wait_recv()

    def forward(slot):
        z = order[slot][0]
        for d in range(1, len(OFFSETS)):
            copy(slot, order.index((z, d)), to_blk(d)).start()

    barrier = pltpu.get_barrier_semaphore()
    peers = [{"walk": lax.rem(w + z, groups)} for z in range(1, groups)]
    reach = sorted({d % owners for d in OFFSETS + tuple(-d for d in OFFSETS)} - {0})
    peers += [{"blk": lax.rem(b + d, owners)} for d in reach]
    for peer in peers:
        pl.semaphore_signal(barrier, inc=1, device_id=peer, device_id_type=pl.DeviceIdType.MESH)

    pack_ref[0, 0:v] = m_in[0, 0]
    times = t_in[0]
    line = lax.broadcasted_iota(jnp.int32, (16, v), 0)
    notes = jnp.where(line == 0, times >> 5, jnp.where(line == 1, times & 31, l_in[0]))
    pack_ref[0, v : v + 16] = notes.astype(jnp.float32).astype(jnp.bfloat16)

    window = own if own % 16 == 0 else (own + 23) // 16 * 16
    first = w * own
    spare = lax.rem(first, 16)
    start = pl.multiple_of(first - spare, 16)

    row = lax.broadcasted_iota(jnp.int32, (nf, v), 0)
    freq = jnp.zeros((nf, v), jnp.int32)
    for f in range(nf):
        freq = jnp.where(row == f, 2 * freq_ref[f] + 1, freq)
    odd[...] = freq
    q = q_ref[0]
    qx = (q * 43) >> 8
    qy = q - SIDE * qx

    scale = 1.0 / (v * v * walkers)
    half = SIDE // 2
    low, high = slice(0, v), slice(v, 2 * v)
    contract = (((1,), (1,)), ((), ()))

    for plain, *_ in (even, odds):
        plain[...] = jnp.zeros_like(plain)

    def prepare(slot, stage):
        plain, turned_m, table, left_s, left_f = stage
        notes = pack_ref[slot, v : v + 16].astype(jnp.float32).astype(jnp.int32)
        times = (notes[0:1] << 5) + notes[1:2]
        labels = notes[2:3]
        sx = (labels * 43) >> 8
        sy = labels - SIDE * sx

        matrix = pack_ref[slot, 0:v]
        plain[low, low] = matrix
        plain[high, high] = matrix
        cu, su = sixth_turn(qx * sx + qy * sy)
        cu = jnp.broadcast_to(cu, (v, v))
        su = jnp.broadcast_to(su, (v, v))
        ct, st = cu.T, su.T
        wide = matrix.astype(jnp.float32) * scale
        re = (wide * (ct * cu + st * su)).astype(jnp.bfloat16)
        im = (wide * (ct * su - st * cu)).astype(jnp.bfloat16)
        turned_m[low, low] = re
        turned_m[high, high] = re
        turned_m[low, high] = im
        turned_m[high, low] = -im

        units = (odd[...] * times) & 2047
        cx, ox = sixth_turn(sx)
        cy, oy = sixth_turn(sy)
        flip_x = (1 - 2 * (sx & 1)).astype(jnp.float32).astype(jnp.bfloat16)
        flip_y = (1 - 2 * (sy & 1)).astype(jnp.float32)
        c, s = sine(units + 512), sine(units)
        for kx in range(half):
            line = [(c, s)]
            for ky in range(1, half):
                c1, s1 = line[-1]
                line.append((c1 * cy + s1 * oy, s1 * cy - c1 * oy))
            line += [(c1 * flip_y, s1 * flip_y) for c1, s1 in line]
            for pair in range(half):
                rows = slice(nf * (SIDE * kx + 2 * pair), nf * (SIDE * kx + 2 * pair + 2))
                far = slice(rows.start + nf * SIDE * half, rows.stop + nf * SIDE * half)
                for side, lanes in enumerate((low, high)):
                    both = jnp.concatenate(
                        [line[2 * pair][side], line[2 * pair + 1][side]], axis=0
                    ).astype(jnp.bfloat16)
                    table[rows, lanes] = both
                    table[far, lanes] = both * flip_x
            c, s = c * cx + s * ox, s * cx - c * ox

        mine = table[pl.ds(start, window), :]
        for ref, wide in (
            (left_s, jnp.dot(mine, turned_m[...], preferred_element_type=jnp.float32)),
            (left_f, lax.dot_general(mine, plain[...], contract, preferred_element_type=jnp.float32)),
        ):
            if window > own:
                wide = jnp.where(spare > 0, wide[8 : 8 + own], wide[:own])
            for tile in range(own // 8):
                part = wide[8 * tile : 8 * tile + 8]
                re, im = part[:, low], part[:, high]
                rows = slice(16 * tile, 16 * tile + 16)
                ref[rows, low] = jnp.concatenate([re, im], axis=0).astype(jnp.bfloat16)
                ref[rows, high] = jnp.concatenate([im, -re], axis=0).astype(jnp.bfloat16)

    def gather_terms(stage, begun=True):
        plain, turned_m, table, left_s, left_f = stage
        for begin in range(0, cols, 256):
            end = min(begin + 256, cols)
            shifted = lax.dot_general(
                left_s[...], table[begin:end], contract, preferred_element_type=jnp.float32
            )
            flipped = lax.dot_general(
                left_f[...], table[begin:end], contract, preferred_element_type=jnp.float32
            )
            for tile in range(own // 8):
                re, im = slice(16 * tile, 16 * tile + 8), slice(16 * tile + 8, 16 * tile + 16)
                rows = slice(8 * tile, 8 * tile + 8)
                sr, si, fr, fi = shifted[re], shifted[im], flipped[re], flipped[im]
                term_re, term_im = sr * fr + si * fi, si * fr - sr * fi
                if begun:
                    out_ref[0, 0, rows, begin:end] += term_re
                    out_ref[0, 1, rows, begin:end] += term_im
                else:
                    out_ref[0, 0, rows, begin:end] = term_re
                    out_ref[0, 1, rows, begin:end] = term_im

    prepare(0, even)
    pl.semaphore_wait(barrier, len(peers))
    for z, d in [o for o in order if o[0] and not o[1]] + [o for o in order if o[1] and not o[0]]:
        copy(0, order.index((z, d)), to_walk(z) if z else to_blk(d)).start()
    gather_terms(even, begun=False)

    turned = lax.rem(b, 2)
    near = len(OFFSETS)
    arrived(1 + turned)
    prepare(1 + turned, odds)

    def step(turn, carry):
        for later, (ready, coming) in enumerate(((odds, even), (even, odds))):
            visit = 2 * turn + 2 + later
            slot = jnp.where(turn == 0, 2 - turned, visit) if later == 0 else visit
            arrived(slot)
            for far in range(near, near + groups - 1):
                if far % 2 == later:
                    @pl.when(turn == (far - 2) // 2)
                    def _(far=far):
                        forward(far)
            if later == 0:
                first_slot = slot
        prepare(first_slot, even)
        gather_terms(odds)
        prepare(visit, odds)
        gather_terms(even)
        return carry

    lax.fori_loop(0, walkers // 2 - 1, step, 0)
    gather_terms(odds)
    for slot in range(1, walkers):
        copy(0, slot, to_walk(1)).wait_send()


def local(walker_m, vertex_times, vertex_labels, freq_index, q_index):
    groups = lax.axis_size("walk")
    owners = lax.axis_size("blk")
    v = walker_m.shape[-1]
    nf = freq_index.shape[0]
    k = SIDE * SIDE * nf
    own = k // groups
    walkers = groups * len(OFFSETS)
    window = own if own % 16 == 0 else (own + 23) // 16 * 16
    held = max(k, max(own * w // 16 * 16 + window for w in range(groups)))
    vmem = pl.BlockSpec(memory_space=pltpu.VMEM)
    smem = pl.BlockSpec(memory_space=pltpu.SMEM)
    bf16 = jnp.bfloat16
    stage = [
        pltpu.VMEM((2 * v, 2 * v), bf16),
        pltpu.VMEM((2 * v, 2 * v), bf16),
        pltpu.VMEM((held, 2 * v), bf16),
        pltpu.VMEM((2 * own, 2 * v), bf16),
        pltpu.VMEM((2 * own, 2 * v), bf16),
    ]
    return pl.pallas_call(
        functools.partial(kernel, groups, owners),
        out_shape=pltpu.VMEM((1, 2, own, k), jnp.float32),
        in_specs=[vmem, vmem, vmem, smem, smem],
        out_specs=vmem,
        scratch_shapes=[
            pltpu.VMEM((walkers, v + 16, v), bf16),
            pltpu.SemaphoreType.DMA((walkers,)),
            pltpu.SemaphoreType.DMA((walkers,)),
            pltpu.VMEM((nf, v), jnp.int32),
            *stage,
            *stage,
        ],
        compiler_params=pltpu.CompilerParams(collective_id=0, has_side_effects=True),
    )(walker_m, vertex_times, vertex_labels, freq_index, q_index)


def solution(mesh):
    return jax.shard_map(
        local,
        mesh=mesh,
        in_specs=(
            P("walk", "blk", None, None),
            P("walk", "blk", None),
            P("walk", "blk", None),
            P(),
            P("blk"),
        ),
        out_specs=P("blk", None, "walk", None),
        check_vma=False,
    )
```

```python
import functools
import math

import jax
import jax.numpy as jnp
from jax import lax
from jax.experimental import pallas as pl
from jax.experimental.pallas import tpu as pltpu
from jax.sharding import PartitionSpec as P

SIDE = 6
TGRID = 1024
OFFSETS = (0, 1, -1, 2)


def sine(units):
    wrapped = ((units + 1024) & 2047) - 1024
    folded = jnp.where(wrapped > 512, 1024 - wrapped, wrapped)
    folded = jnp.where(wrapped < -512, -1024 - wrapped, folded)
    x = folded.astype(jnp.float32) * (math.pi / 1024.0)
    y = x * x
    total = jnp.full_like(y, 1.0 / math.factorial(13))
    for order in (11, 9, 7, 5, 3, 1):
        sign = -1.0 if (order // 2) % 2 else 1.0
        total = total * y + sign / math.factorial(order)
    return total * x


def sixth_turn(m):
    r = m - 6 * ((m * 10923) >> 16)
    half = jnp.where((r == 1) | (r == 5), 0.5, -0.5)
    cosine = jnp.where(r == 0, 1.0, jnp.where(r == 3, -1.0, half))
    root = math.sqrt(3.0) / 2.0
    side = jnp.where(r < 3, root, -root)
    return cosine.astype(jnp.float32), jnp.where((r == 0) | (r == 3), 0.0, side).astype(jnp.float32)


def visits(groups):
    rest = range(1, len(OFFSETS))
    far = [(z, 0) for z in range(1, groups)]
    start = [(0, 0), (0, 1), (0, 2)] + far[:1] + [(0, 3)] + far[1:]
    return start + [(z, d) for z in range(1, groups) for d in rest]


def across(w, z, groups):
    if groups & (groups - 1):
        return lax.rem(w + groups - z, groups)
    bit, there = 1, w
    while bit < groups:
        if z & bit:
            there = there + bit - 2 * bit * lax.rem(w // bit, 2)
        bit *= 2
    return there


def kernel(
    groups, owners, m_in, t_in, l_in, freq_ref, q_ref, out_ref,
    pack_ref, send_sem, recv_sem, odd, *stages,
):
    order = visits(groups)
    walkers = len(order)
    w = lax.axis_index("walk")
    b = lax.axis_index("blk")
    v = m_in.shape[-1]
    nf = freq_ref.shape[0]
    own = out_ref.shape[2]
    cols = out_ref.shape[3]
    even, odds = stages[: len(stages) // 2], stages[len(stages) // 2 :]

    def place(z, d):
        where = {"blk": lax.rem(b + owners - OFFSETS[d], owners)} if d else {}
        return where | ({"walk": across(w, z, groups)} if z else {})

    def copy(source, slot, device):
        return pltpu.make_async_remote_copy(
            src_ref=pack_ref.at[source],
            dst_ref=pack_ref.at[slot],
            send_sem=send_sem.at[slot],
            recv_sem=recv_sem.at[slot],
            device_id=device,
            device_id_type=pl.DeviceIdType.MESH,
        )

    def arrived(slot):
        copy(0, slot, place(1, 0)).wait_recv()

    def forward(slot):
        z = order[slot][0]
        for d in range(1, len(OFFSETS)):
            copy(slot, order.index((z, d)), place(0, d)).start()

    barrier = pltpu.get_barrier_semaphore()
    peers = [{"walk": lax.rem(w + z, groups)} for z in range(1, groups)]
    reach = sorted({d % owners for d in OFFSETS + tuple(-d for d in OFFSETS)} - {0})
    peers += [{"blk": lax.rem(b + d, owners)} for d in reach]
    beside = [across(w, 1, groups)] + ([lax.rem(w + 1, groups)] if groups & (groups - 1) else [])
    peers += [{"blk": lax.rem(b + d, owners), "walk": z} for d in reach for z in beside]
    for peer in peers:
        pl.semaphore_signal(barrier, inc=1, device_id=peer, device_id_type=pl.DeviceIdType.MESH)

    pack_ref[0, 0:v] = m_in[0, 0]
    times = t_in[0]
    line = lax.broadcasted_iota(jnp.int32, (16, v), 0)
    notes = jnp.where(line == 0, times >> 5, jnp.where(line == 1, times & 31, l_in[0]))
    pack_ref[0, v : v + 16] = notes.astype(jnp.float32).astype(jnp.bfloat16)

    window = own if own % 16 == 0 else (own + 23) // 16 * 16
    first = w * own
    spare = lax.rem(first, 16)
    start = pl.multiple_of(first - spare, 16)

    row = lax.broadcasted_iota(jnp.int32, (nf, v), 0)
    freq = jnp.zeros((nf, v), jnp.int32)
    for f in range(nf):
        freq = jnp.where(row == f, 2 * freq_ref[f] + 1, freq)
    odd[...] = freq
    q = q_ref[0]
    qx = (q * 43) >> 8
    qy = q - SIDE * qx

    scale = 1.0 / (v * v * walkers)
    half = SIDE // 2
    low, high = slice(0, v), slice(v, 2 * v)
    contract = (((1,), (1,)), ((), ()))

    for plain, *_ in (even, odds):
        plain[...] = jnp.zeros_like(plain)

    def prepare(slot, stage):
        plain, turned_m, table, left_s, left_f = stage
        notes = pack_ref[slot, v : v + 16].astype(jnp.float32).astype(jnp.int32)
        times = (notes[0:1] << 5) + notes[1:2]
        labels = notes[2:3]
        sx = (labels * 43) >> 8
        sy = labels - SIDE * sx

        matrix = pack_ref[slot, 0:v]
        plain[low, low] = matrix
        plain[high, high] = matrix
        cu, su = sixth_turn(qx * sx + qy * sy)
        cu = jnp.broadcast_to(cu, (v, v))
        su = jnp.broadcast_to(su, (v, v))
        ct, st = cu.T, su.T
        wide = matrix.astype(jnp.float32) * scale
        re = (wide * (ct * cu + st * su)).astype(jnp.bfloat16)
        im = (wide * (ct * su - st * cu)).astype(jnp.bfloat16)
        turned_m[low, low] = re
        turned_m[high, high] = re
        turned_m[low, high] = im
        turned_m[high, low] = -im

        units = (odd[...] * times) & 2047
        cx, ox = sixth_turn(sx)
        cy, oy = sixth_turn(sy)
        flip_x = (1 - 2 * (sx & 1)).astype(jnp.float32).astype(jnp.bfloat16)
        flip_y = (1 - 2 * (sy & 1)).astype(jnp.float32)
        c, s = sine(units + 512), sine(units)
        for kx in range(half):
            line = [(c, s)]
            for ky in range(1, half):
                c1, s1 = line[-1]
                line.append((c1 * cy + s1 * oy, s1 * cy - c1 * oy))
            line += [(c1 * flip_y, s1 * flip_y) for c1, s1 in line]
            for pair in range(half):
                rows = slice(nf * (SIDE * kx + 2 * pair), nf * (SIDE * kx + 2 * pair + 2))
                far = slice(rows.start + nf * SIDE * half, rows.stop + nf * SIDE * half)
                for side, lanes in enumerate((low, high)):
                    both = jnp.concatenate(
                        [line[2 * pair][side], line[2 * pair + 1][side]], axis=0
                    ).astype(jnp.bfloat16)
                    table[rows, lanes] = both
                    table[far, lanes] = both * flip_x
            c, s = c * cx + s * ox, s * cx - c * ox

        mine = table[pl.ds(start, window), :]
        for ref, wide in (
            (left_s, jnp.dot(mine, turned_m[...], preferred_element_type=jnp.float32)),
            (left_f, lax.dot_general(mine, plain[...], contract, preferred_element_type=jnp.float32)),
        ):
            if window > own:
                wide = jnp.where(spare > 0, wide[8 : 8 + own], wide[:own])
            for tile in range(own // 8):
                part = wide[8 * tile : 8 * tile + 8]
                re, im = part[:, low], part[:, high]
                rows = slice(16 * tile, 16 * tile + 16)
                ref[rows, low] = jnp.concatenate([re, im], axis=0).astype(jnp.bfloat16)
                ref[rows, high] = jnp.concatenate([im, -re], axis=0).astype(jnp.bfloat16)

    def gather_terms(stage, begun=True):
        plain, turned_m, table, left_s, left_f = stage
        for begin in range(0, cols, 256):
            end = min(begin + 256, cols)
            shifted = lax.dot_general(
                left_s[...], table[begin:end], contract, preferred_element_type=jnp.float32
            )
            flipped = lax.dot_general(
                left_f[...], table[begin:end], contract, preferred_element_type=jnp.float32
            )
            for tile in range(own // 8):
                re, im = slice(16 * tile, 16 * tile + 8), slice(16 * tile + 8, 16 * tile + 16)
                rows = slice(8 * tile, 8 * tile + 8)
                sr, si, fr, fi = shifted[re], shifted[im], flipped[re], flipped[im]
                term_re, term_im = sr * fr + si * fi, si * fr - sr * fi
                if begun:
                    out_ref[0, 0, rows, begin:end] += term_re
                    out_ref[0, 1, rows, begin:end] += term_im
                else:
                    out_ref[0, 0, rows, begin:end] = term_re
                    out_ref[0, 1, rows, begin:end] = term_im

    prepare(0, even)
    pl.semaphore_wait(barrier, len(peers))
    for slot, (z, d) in enumerate(order):
        if slot and (not z or not d or z == 1):
            copy(0, slot, place(z, d)).start()
    gather_terms(even, begun=False)

    turned = lax.rem(b, 2)
    arrived(1 + turned)
    prepare(1 + turned, odds)

    def step(turn, carry):
        for later, (ready, coming) in enumerate(((odds, even), (even, odds))):
            visit = 2 * turn + 2 + later
            slot = jnp.where(turn == 0, 2 - turned, visit) if later == 0 else visit
            arrived(slot)
            for relay, (z, d) in enumerate(order):
                if z > 1 and not d and relay % 2 == later:
                    @pl.when(turn == (relay - 2) // 2)
                    def _(relay=relay):
                        forward(relay)
            if later == 0:
                first_slot = slot
        prepare(first_slot, even)
        gather_terms(odds)
        prepare(visit, odds)
        gather_terms(even)
        return carry

    lax.fori_loop(0, walkers // 2 - 1, step, 0)
    gather_terms(odds)
    for slot in range(1, walkers):
        copy(0, slot, place(1, 0)).wait_send()


def local(walker_m, vertex_times, vertex_labels, freq_index, q_index):
    groups = lax.axis_size("walk")
    owners = lax.axis_size("blk")
    v = walker_m.shape[-1]
    nf = freq_index.shape[0]
    k = SIDE * SIDE * nf
    own = k // groups
    walkers = groups * len(OFFSETS)
    window = own if own % 16 == 0 else (own + 23) // 16 * 16
    held = max(k, max(own * w // 16 * 16 + window for w in range(groups)))
    vmem = pl.BlockSpec(memory_space=pltpu.VMEM)
    smem = pl.BlockSpec(memory_space=pltpu.SMEM)
    bf16 = jnp.bfloat16
    stage = [
        pltpu.VMEM((2 * v, 2 * v), bf16),
        pltpu.VMEM((2 * v, 2 * v), bf16),
        pltpu.VMEM((held, 2 * v), bf16),
        pltpu.VMEM((2 * own, 2 * v), bf16),
        pltpu.VMEM((2 * own, 2 * v), bf16),
    ]
    return pl.pallas_call(
        functools.partial(kernel, groups, owners),
        out_shape=pltpu.VMEM((1, 2, own, k), jnp.float32),
        in_specs=[vmem, vmem, vmem, smem, smem],
        out_specs=vmem,
        scratch_shapes=[
            pltpu.VMEM((walkers, v + 16, v), bf16),
            pltpu.SemaphoreType.DMA((walkers,)),
            pltpu.SemaphoreType.DMA((walkers,)),
            pltpu.VMEM((nf, v), jnp.int32),
            *stage,
            *stage,
        ],
        compiler_params=pltpu.CompilerParams(collective_id=0, has_side_effects=True),
    )(walker_m, vertex_times, vertex_labels, freq_index, q_index)


def solution(mesh):
    return jax.shard_map(
        local,
        mesh=mesh,
        in_specs=(
            P("walk", "blk", None, None),
            P("walk", "blk", None),
            P("walk", "blk", None),
            P(),
            P("blk"),
        ),
        out_specs=P("blk", None, "walk", None),
        check_vma=False,
    )
```

```python
import functools
import math

import jax
import jax.numpy as jnp
from jax import lax
from jax.experimental import pallas as pl
from jax.experimental.pallas import tpu as pltpu
from jax.sharding import PartitionSpec as P

SIDE = 6
TGRID = 1024
OFFSETS = (0, 1, -1, 2)
EVERY = 2
SENDS = ((0, 1), (0, 2), (1, 0), (0, 3), (2, 0), (3, 0))
PLAN = (0, 0, 0, 0)


def sine(units):
    wrapped = ((units + 1024) & 2047) - 1024
    folded = jnp.where(wrapped > 512, 1024 - wrapped, wrapped)
    folded = jnp.where(wrapped < -512, -1024 - wrapped, folded)
    x = folded.astype(jnp.float32) * (math.pi / 1024.0)
    y = x * x
    total = jnp.full_like(y, 1.0 / math.factorial(13))
    for order in (11, 9, 7, 5, 3, 1):
        sign = -1.0 if (order // 2) % 2 else 1.0
        total = total * y + sign / math.factorial(order)
    return total * x


def sixth_turn(m):
    r = m - 6 * ((m * 10923) >> 16)
    half = jnp.where((r == 1) | (r == 5), 0.5, -0.5)
    cosine = jnp.where(r == 0, 1.0, jnp.where(r == 3, -1.0, half))
    root = math.sqrt(3.0) / 2.0
    side = jnp.where(r < 3, root, -root)
    return cosine.astype(jnp.float32), jnp.where((r == 0) | (r == 3), 0.0, side).astype(jnp.float32)


def visits(groups):
    order = [(0, 0), (0, "p"), (0, "c"), (1, 0), (0, 3), (1, "p")]
    order += [(z, 0) for z in range(2, groups)] + [(1, "c"), (1, 3)]
    order += [(z, "p") for z in range(2, groups)]
    return order + [(z, d) for z in range(2, groups) for d in ("c", 3)]


def across(w, z, groups):
    if groups & (groups - 1):
        return lax.rem(w + groups - z, groups)
    bit, there = 1, w
    while bit < groups:
        if z & bit:
            there = there + bit - 2 * bit * lax.rem(w // bit, 2)
        bit *= 2
    return there


def kernel(
    groups, owners, m_in, t_in, l_in, freq_ref, q_ref, out_ref,
    pack_ref, send_sem, recv_sem, odd, *stages,
):
    walkers = groups * len(OFFSETS)
    order = [(z, d) for z in range(groups) for d in range(len(OFFSETS))]
    w = lax.axis_index("walk")
    b = lax.axis_index("blk")
    v = m_in.shape[-1]
    nf = freq_ref.shape[0]
    own = out_ref.shape[2]
    cols = out_ref.shape[3]
    even, odds = stages[: len(stages) // 2], stages[len(stages) // 2 :]

    def place(z, d):
        where = {"blk": lax.rem(b + owners - OFFSETS[d], owners)} if d else {}
        return where | ({"walk": across(w, z, groups)} if z else {})

    def copy(source, slot, device):
        return pltpu.make_async_remote_copy(
            src_ref=pack_ref.at[source],
            dst_ref=pack_ref.at[slot],
            send_sem=send_sem.at[slot],
            recv_sem=recv_sem.at[slot],
            device_id=device,
            device_id_type=pl.DeviceIdType.MESH,
        )

    def arrived(slot):
        copy(0, slot, place(1, 0)).wait_recv()

    def forward(z):
        for d in range(1, len(OFFSETS)):
            copy(order.index((z, 0)), order.index((z, d)), place(0, d)).start()

    barrier = pltpu.get_barrier_semaphore()
    peers = [{"walk": lax.rem(w + z, groups)} for z in range(1, groups)]
    reach = sorted({d % owners for d in OFFSETS + tuple(-d for d in OFFSETS)} - {0})
    peers += [{"blk": lax.rem(b + d, owners)} for d in reach]
    for peer in peers:
        pl.semaphore_signal(barrier, inc=1, device_id=peer, device_id_type=pl.DeviceIdType.MESH)

    pack_ref[0, 0:v] = m_in[0, 0]
    times = t_in[0]
    line = lax.broadcasted_iota(jnp.int32, (16, v), 0)
    notes = jnp.where(line == 0, times >> 5, jnp.where(line == 1, times & 31, l_in[0]))
    pack_ref[0, v : v + 16] = notes.astype(jnp.float32).astype(jnp.bfloat16)

    window = own if own % 16 == 0 else (own + 23) // 16 * 16
    first = w * own
    spare = lax.rem(first, 16)
    start = pl.multiple_of(first - spare, 16)

    row = lax.broadcasted_iota(jnp.int32, (nf, v), 0)
    freq = jnp.zeros((nf, v), jnp.int32)
    for f in range(nf):
        freq = jnp.where(row == f, 2 * freq_ref[f] + 1, freq)
    odd[...] = freq
    q = q_ref[0]
    qx = (q * 43) >> 8
    qy = q - SIDE * qx

    scale = 1.0 / (v * v * walkers)
    half = SIDE // 2
    low, high = slice(0, v), slice(v, 2 * v)
    contract = (((1,), (1,)), ((), ()))

    for plain, *_ in (even, odds):
        plain[...] = jnp.zeros_like(plain)

    def prepare(slot, stage):
        plain, turned_m, table, left_s, left_f = stage
        notes = pack_ref[slot, v : v + 16].astype(jnp.float32).astype(jnp.int32)
        times = (notes[0:1] << 5) + notes[1:2]
        labels = notes[2:3]
        sx = (labels * 43) >> 8
        sy = labels - SIDE * sx

        matrix = pack_ref[slot, 0:v]
        plain[low, low] = matrix
        plain[high, high] = matrix
        cu, su = sixth_turn(qx * sx + qy * sy)
        cu = jnp.broadcast_to(cu, (v, v))
        su = jnp.broadcast_to(su, (v, v))
        ct, st = cu.T, su.T
        wide = matrix.astype(jnp.float32) * scale
        re = (wide * (ct * cu + st * su)).astype(jnp.bfloat16)
        im = (wide * (ct * su - st * cu)).astype(jnp.bfloat16)
        turned_m[low, low] = re
        turned_m[high, high] = re
        turned_m[low, high] = im
        turned_m[high, low] = -im

        yield
        units = (odd[...] * times) & 2047
        cx, ox = sixth_turn(sx)
        cy, oy = sixth_turn(sy)
        flip_x = (1 - 2 * (sx & 1)).astype(jnp.float32).astype(jnp.bfloat16)
        flip_y = (1 - 2 * (sy & 1)).astype(jnp.float32)
        c, s = sine(units + 512), sine(units)
        for kx in range(half):
            line = [(c, s)]
            for ky in range(1, half):
                c1, s1 = line[-1]
                line.append((c1 * cy + s1 * oy, s1 * cy - c1 * oy))
            line += [(c1 * flip_y, s1 * flip_y) for c1, s1 in line]
            for pair in range(half):
                rows = slice(nf * (SIDE * kx + 2 * pair), nf * (SIDE * kx + 2 * pair + 2))
                far = slice(rows.start + nf * SIDE * half, rows.stop + nf * SIDE * half)
                for side, lanes in enumerate((low, high)):
                    both = jnp.concatenate(
                        [line[2 * pair][side], line[2 * pair + 1][side]], axis=0
                    ).astype(jnp.bfloat16)
                    table[rows, lanes] = both
                    table[far, lanes] = both * flip_x
            c, s = c * cx + s * ox, s * cx - c * ox
            yield

        mine = table[pl.ds(start, window), :]
        for ref, wide in (
            (left_s, jnp.dot(mine, turned_m[...], preferred_element_type=jnp.float32)),
            (left_f, lax.dot_general(mine, plain[...], contract, preferred_element_type=jnp.float32)),
        ):
            if window > own:
                wide = jnp.where(spare > 0, wide[8 : 8 + own], wide[:own])
            for tile in range(own // 8):
                part = wide[8 * tile : 8 * tile + 8]
                re, im = part[:, low], part[:, high]
                rows = slice(16 * tile, 16 * tile + 16)
                ref[rows, low] = jnp.concatenate([re, im], axis=0).astype(jnp.bfloat16)
                ref[rows, high] = jnp.concatenate([im, -re], axis=0).astype(jnp.bfloat16)
            yield

    def gather_terms(stage, begun=True):
        plain, turned_m, table, left_s, left_f = stage
        for begin in range(0, cols, 256):
            end = min(begin + 256, cols)
            shifted = lax.dot_general(
                left_s[...], table[begin:end], contract, preferred_element_type=jnp.float32
            )
            flipped = lax.dot_general(
                left_f[...], table[begin:end], contract, preferred_element_type=jnp.float32
            )
            for tile in range(own // 8):
                re, im = slice(16 * tile, 16 * tile + 8), slice(16 * tile + 8, 16 * tile + 16)
                rows = slice(8 * tile, 8 * tile + 8)
                sr, si, fr, fi = shifted[re], shifted[im], flipped[re], flipped[im]
                term_re, term_im = sr * fr + si * fi, si * fr - sr * fi
                if begun:
                    out_ref[0, 0, rows, begin:end] += term_re
                    out_ref[0, 1, rows, begin:end] += term_im
                else:
                    out_ref[0, 0, rows, begin:end] = term_re
                    out_ref[0, 1, rows, begin:end] = term_im
            yield

    def run(plan, *parts):
        for part in plan:
            next(parts[part], None)
        for part in parts:
            for _ in part:
                pass

    turned = lax.rem(b, 2)

    def held(visit):
        z, d = plan[visit]
        d = {"p": 1 + turned, "c": 2 - turned}.get(d, d)
        return z * len(OFFSETS) + d

    def await_visits(*coming):
        for visit in coming:
            if visit < walkers:
                arrived(held(visit))
                z, d = plan[visit]
                if z and not d:
                    forward(z)

    plan = visits(groups)
    run((), prepare(0, even))
    pl.semaphore_wait(barrier, len(peers))
    for z, d in SENDS:
        if z < groups:
            copy(0, order.index((z, d)), place(z, d)).start()
    run((), gather_terms(even, begun=False))
    await_visits(1)
    run((), prepare(held(1), odds))
    for visit in range(2, walkers, EVERY):
        await_visits(*range(visit, min(visit + EVERY, walkers)))
        for coming in range(visit, min(visit + EVERY, walkers)):
            now, then = (odds, even) if coming % 2 == 0 else (even, odds)
            run(PLAN, gather_terms(now), prepare(held(coming), then))
    run((), gather_terms(odds))
    for slot in range(1, walkers):
        copy(0, slot, place(1, 0)).wait_send()


def local(walker_m, vertex_times, vertex_labels, freq_index, q_index):
    groups = lax.axis_size("walk")
    owners = lax.axis_size("blk")
    v = walker_m.shape[-1]
    nf = freq_index.shape[0]
    k = SIDE * SIDE * nf
    own = k // groups
    walkers = groups * len(OFFSETS)
    window = own if own % 16 == 0 else (own + 23) // 16 * 16
    held = max(k, max(own * w // 16 * 16 + window for w in range(groups)))
    vmem = pl.BlockSpec(memory_space=pltpu.VMEM)
    smem = pl.BlockSpec(memory_space=pltpu.SMEM)
    bf16 = jnp.bfloat16
    stage = [
        pltpu.VMEM((2 * v, 2 * v), bf16),
        pltpu.VMEM((2 * v, 2 * v), bf16),
        pltpu.VMEM((held, 2 * v), bf16),
        pltpu.VMEM((2 * own, 2 * v), bf16),
        pltpu.VMEM((2 * own, 2 * v), bf16),
    ]
    return pl.pallas_call(
        functools.partial(kernel, groups, owners),
        out_shape=pltpu.VMEM((1, 2, own, k), jnp.float32),
        in_specs=[vmem, vmem, vmem, smem, smem],
        out_specs=vmem,
        scratch_shapes=[
            pltpu.VMEM((walkers, v + 16, v), bf16),
            pltpu.SemaphoreType.DMA((walkers,)),
            pltpu.SemaphoreType.DMA((walkers,)),
            pltpu.VMEM((nf, v), jnp.int32),
            *stage,
            *stage,
        ],
        compiler_params=pltpu.CompilerParams(collective_id=0, has_side_effects=True),
    )(walker_m, vertex_times, vertex_labels, freq_index, q_index)


def solution(mesh):
    return jax.shard_map(
        local,
        mesh=mesh,
        in_specs=(
            P("walk", "blk", None, None),
            P("walk", "blk", None),
            P("walk", "blk", None),
            P(),
            P("blk"),
        ),
        out_specs=P("blk", None, "walk", None),
        check_vma=False,
    )
```

```python
import functools
import math

import jax
import jax.numpy as jnp
from jax import lax
from jax.experimental import pallas as pl
from jax.experimental.pallas import tpu as pltpu
from jax.sharding import PartitionSpec as P

SIDE = 6
TGRID = 1024
OFFSETS = (0, 1, -1, 2)


def sine(units):
    wrapped = ((units + 1024) & 2047) - 1024
    folded = jnp.where(wrapped > 512, 1024 - wrapped, wrapped)
    folded = jnp.where(wrapped < -512, -1024 - wrapped, folded)
    x = folded.astype(jnp.float32) * (math.pi / 1024.0)
    y = x * x
    total = jnp.full_like(y, 1.0 / math.factorial(13))
    for order in (11, 9, 7, 5, 3, 1):
        sign = -1.0 if (order // 2) % 2 else 1.0
        total = total * y + sign / math.factorial(order)
    return total * x


def sixth_turn(m):
    r = m - 6 * ((m * 10923) >> 16)
    half = jnp.where((r == 1) | (r == 5), 0.5, -0.5)
    cosine = jnp.where(r == 0, 1.0, jnp.where(r == 3, -1.0, half))
    root = math.sqrt(3.0) / 2.0
    side = jnp.where(r < 3, root, -root)
    return cosine.astype(jnp.float32), jnp.where((r == 0) | (r == 3), 0.0, side).astype(jnp.float32)


def visits(groups):
    order = [(0, 0), (0, "p"), (1, 0), (0, "c"), (1, "p")]
    order += [(z, 0) for z in range(2, min(groups, 3))] + [(0, 3)]
    order += [(z, 0) for z in range(3, groups)] + [(1, "c"), (1, 3)]
    order += [(z, "p") for z in range(2, groups)] + [(z, "c") for z in range(2, groups)]
    return order + [(z, 3) for z in range(2, groups)]


def blocks(walkers):
    out = [((1,), "T1 L1 G1"), ((2,), "T2 L2"), ((3,), "g2 g2 T3 L3 G2")]
    out.append(((4, 5), "g3 g3 g3 T4 L4 G3 g4 g4 g4 T5 L5 G4"))
    out.append(((6, 7, 8), "g5 g5 g5 T6 L6 G5 T7 g6 g6 L7 G6 T8"))
    done, ready = 6, 9
    while done < walkers - 1:
        coming = tuple(range(ready, min(ready + 2, walkers)))
        ops = []
        for step in range(2 if ready + 2 <= walkers else walkers - 1 - done):
            done += 1
            ops += [f"g{done}"] * 1 + [f"L{done + 1}"] * (done + 1 < walkers) + [f"T{done + 2}"] * (done + 2 < walkers) + [f"G{done}"]
        ready += len(coming)
        out.append((coming, " ".join(ops)))
    return out


def across(w, z, groups):
    if groups & (groups - 1):
        return lax.rem(w + groups - z, groups)
    bit, there = 1, w
    while bit < groups:
        if z & bit:
            there = there + bit - 2 * bit * lax.rem(w // bit, 2)
        bit *= 2
    return there


def kernel(
    groups, owners, m_in, t_in, l_in, freq_ref, q_ref, out_ref,
    pack_ref, send_sem, recv_sem, relay_sem, odd, *stages,
):
    walkers = groups * len(OFFSETS)
    order = [(z, d) for z in range(groups) for d in range(len(OFFSETS))]
    w = lax.axis_index("walk")
    b = lax.axis_index("blk")
    v = m_in.shape[-1]
    nf = freq_ref.shape[0]
    own = out_ref.shape[2]
    cols = out_ref.shape[3]
    tables = [stages[3 * i : 3 * i + 3] for i in range(3)]
    lefts = [stages[9 + 2 * i : 11 + 2 * i] for i in range(2)]

    def place(z, d):
        where = {"blk": lax.rem(b + owners - OFFSETS[d], owners)} if d else {}
        return where | ({"walk": across(w, z, groups)} if z else {})

    turned = lax.rem(b, 2)
    beside = {"blk": b + 1 - 2 * turned}

    def copy(source, slot, device, sent=None):
        return pltpu.make_async_remote_copy(
            src_ref=pack_ref.at[source],
            dst_ref=pack_ref.at[slot],
            send_sem=send_sem.at[slot] if sent is None else relay_sem.at[sent],
            recv_sem=recv_sem.at[slot],
            device_id=device,
            device_id_type=pl.DeviceIdType.MESH,
        )

    def arrived(slot):
        copy(0, slot, place(1, 0)).wait_recv()

    def relay(z):
        return copy(order.index((z, 1)), order.index((z, 3)), beside, z)

    def spread(z):
        here = order.index((z, 0))
        for d in (1, 2):
            copy(here, order.index((z, d)), place(0, d)).start()

        @pl.when(turned == 1)
        def _():
            copy(here, order.index((z, 3)), place(0, 3)).start()

    barrier = pltpu.get_barrier_semaphore()
    peers = [{"walk": lax.rem(w + z, groups)} for z in range(1, groups)]
    reach = sorted({d % owners for d in OFFSETS + tuple(-d for d in OFFSETS)} - {0})
    peers += [{"blk": lax.rem(b + d, owners)} for d in reach]
    for peer in peers:
        pl.semaphore_signal(barrier, inc=1, device_id=peer, device_id_type=pl.DeviceIdType.MESH)

    pack_ref[0, 0:v] = m_in[0, 0]
    times = t_in[0]
    line = lax.broadcasted_iota(jnp.int32, (8, v), 0)
    notes = jnp.where(line == 0, times >> 5, jnp.where(line == 1, times & 31, l_in[0]))
    pack_ref[0, v : v + 8] = notes.astype(jnp.float32).astype(jnp.bfloat16)

    window = own if own % 16 == 0 else (own + 23) // 16 * 16
    first = w * own
    spare = lax.rem(first, 16)
    start = pl.multiple_of(first - spare, 16)

    row = lax.broadcasted_iota(jnp.int32, (nf, v), 0)
    freq = jnp.zeros((nf, v), jnp.int32)
    for f in range(nf):
        freq = jnp.where(row == f, 2 * freq_ref[f] + 1, freq)
    odd[...] = freq
    q = q_ref[0]
    qx = (q * 43) >> 8
    qy = q - SIDE * qx

    scale = 1.0 / (v * v * walkers)
    half = SIDE // 2
    low, high = slice(0, v), slice(v, 2 * v)
    contract = (((1,), (1,)), ((), ()))

    for plain, _, _ in tables:
        plain[...] = jnp.zeros_like(plain)
    def tabulate(visit):
        slot = held(visit)
        plain, turned_m, table = tables[visit % len(tables)]
        notes = pack_ref[slot, v : v + 8].astype(jnp.float32).astype(jnp.int32)
        times = (notes[0:1] << 5) + notes[1:2]
        labels = notes[2:3]
        sx = (labels * 43) >> 8
        sy = labels - SIDE * sx

        matrix = pack_ref[slot, 0:v]
        plain[low, low] = matrix
        plain[high, high] = matrix
        cu, su = sixth_turn(qx * sx + qy * sy)
        cu = jnp.broadcast_to(cu, (v, v))
        su = jnp.broadcast_to(su, (v, v))
        ct, st = cu.T, su.T
        wide = matrix.astype(jnp.float32) * scale
        re = (wide * (ct * cu + st * su)).astype(jnp.bfloat16)
        im = (wide * (ct * su - st * cu)).astype(jnp.bfloat16)
        turned_m[low, low] = re
        turned_m[high, high] = re
        turned_m[low, high] = im
        turned_m[high, low] = -im

        units = (odd[...] * times) & 2047
        cx, ox = sixth_turn(sx)
        cy, oy = sixth_turn(sy)
        flip_x = (1 - 2 * (sx & 1)).astype(jnp.float32).astype(jnp.bfloat16)
        flip_y = (1 - 2 * (sy & 1)).astype(jnp.float32)
        c, s = sine(units + 512), sine(units)
        for kx in range(half):
            line = [(c, s)]
            for ky in range(1, half):
                c1, s1 = line[-1]
                line.append((c1 * cy + s1 * oy, s1 * cy - c1 * oy))
            line += [(c1 * flip_y, s1 * flip_y) for c1, s1 in line]
            for pair in range(half):
                rows = slice(nf * (SIDE * kx + 2 * pair), nf * (SIDE * kx + 2 * pair + 2))
                far = slice(rows.start + nf * SIDE * half, rows.stop + nf * SIDE * half)
                for side, lanes in enumerate((low, high)):
                    both = jnp.concatenate(
                        [line[2 * pair][side], line[2 * pair + 1][side]], axis=0
                    ).astype(jnp.bfloat16)
                    table[rows, lanes] = both
                    table[far, lanes] = both * flip_x
            c, s = c * cx + s * ox, s * cx - c * ox

    def lift(visit):
        plain, turned_m, table = tables[visit % len(tables)]
        left_s, left_f = lefts[visit % len(lefts)]
        mine = table[pl.ds(start, window), :]
        for ref, wide in (
            (left_s, jnp.dot(mine, turned_m[...], preferred_element_type=jnp.float32)),
            (left_f, lax.dot_general(mine, plain[...], contract, preferred_element_type=jnp.float32)),
        ):
            if window > own:
                wide = jnp.where(spare > 0, wide[8 : 8 + own], wide[:own])
            for tile in range(own // 8):
                part = wide[8 * tile : 8 * tile + 8]
                re, im = part[:, low], part[:, high]
                rows = slice(16 * tile, 16 * tile + 16)
                ref[rows, low] = jnp.concatenate([re, im], axis=0).astype(jnp.bfloat16)
                ref[rows, high] = jnp.concatenate([im, -re], axis=0).astype(jnp.bfloat16)

    def gather_terms(visit):
        table = tables[visit % len(tables)][2]
        left_s, left_f = lefts[visit % len(lefts)]
        begun = visit > 0

        def add(ref, place, term):
            if begun:
                ref[place] += term
            else:
                ref[place] = term

        for begin in range(0, cols, 256):
            end = min(begin + 256, cols)
            shifted = lax.dot_general(
                left_s[...], table[begin:end], contract, preferred_element_type=jnp.float32
            )
            flipped = lax.dot_general(
                left_f[...], table[begin:end], contract, preferred_element_type=jnp.float32
            )
            for tile in range(own // 8):
                re, im = slice(16 * tile, 16 * tile + 8), slice(16 * tile + 8, 16 * tile + 16)
                rows = slice(8 * tile, 8 * tile + 8)
                sr, si, fr, fi = shifted[re], shifted[im], flipped[re], flipped[im]
                add(out_ref, (0, 0, rows, slice(begin, end)), sr * fr + si * fi)
                add(out_ref, (0, 1, rows, slice(begin, end)), si * fr - sr * fi)
            yield

    def held(visit):
        z, d = plan[visit]
        d = {"p": 1 + turned, "c": 2 - turned}.get(d, d)
        return z * len(OFFSETS) + d

    def await_visits(coming):
        for visit in coming:
            arrived(held(visit))
            z, d = plan[visit]
            if z and not d:
                spread(z)
            if d == "c":
                @pl.when(turned == 1)
                def _(z=z):
                    relay(z).start()

    plan = visits(groups)
    gathers = {}

    def run(ops):
        for op in ops.split():
            kind, visit = op[0], int(op[1:])
            if kind == "T":
                tabulate(visit)
            elif kind == "L":
                lift(visit)
            else:
                gathers.setdefault(visit, gather_terms(visit))
                for _ in gathers[visit]:
                    if kind == "g":
                        break

    pl.semaphore_wait(barrier, len(peers))
    for z in range(1, groups):
        if z == 2:
            spread(0)
        copy(0, order.index((z, 0)), place(z, 0)).start()
    if groups == 2:
        spread(0)
    run("T0 L0 G0")
    for coming, ops in blocks(walkers):
        await_visits(coming)
        run(ops)
    for slot, (z, d) in enumerate(order):
        if slot and d != 3:
            copy(0, slot, place(1, 0)).wait_send()

    @pl.when(turned == 1)
    def _():
        for z in range(groups):
            copy(0, order.index((z, 3)), place(1, 0)).wait_send()
            relay(z).wait_send()


def local(walker_m, vertex_times, vertex_labels, freq_index, q_index):
    groups = lax.axis_size("walk")
    owners = lax.axis_size("blk")
    v = walker_m.shape[-1]
    nf = freq_index.shape[0]
    k = SIDE * SIDE * nf
    own = k // groups
    walkers = groups * len(OFFSETS)
    window = own if own % 16 == 0 else (own + 23) // 16 * 16
    held = max(k, max(own * w // 16 * 16 + window for w in range(groups)))
    vmem = pl.BlockSpec(memory_space=pltpu.VMEM)
    smem = pl.BlockSpec(memory_space=pltpu.SMEM)
    bf16 = jnp.bfloat16
    table = [
        pltpu.VMEM((2 * v, 2 * v), bf16),
        pltpu.VMEM((2 * v, 2 * v), bf16),
        pltpu.VMEM((held, 2 * v), bf16),
    ]
    left = [
        pltpu.VMEM((2 * own, 2 * v), bf16),
        pltpu.VMEM((2 * own, 2 * v), bf16),
    ]
    return pl.pallas_call(
        functools.partial(kernel, groups, owners),
        out_shape=pltpu.VMEM((1, 2, own, k), jnp.float32),
        in_specs=[vmem, vmem, vmem, smem, smem],
        out_specs=vmem,
        scratch_shapes=[
            pltpu.VMEM((walkers, v + 8, v), bf16),
            pltpu.SemaphoreType.DMA((walkers,)),
            pltpu.SemaphoreType.DMA((walkers,)),
            pltpu.SemaphoreType.DMA((groups,)),
            pltpu.VMEM((nf, v), jnp.int32),
            *table * 3,
            *left * 2,
        ],
        compiler_params=pltpu.CompilerParams(collective_id=0, has_side_effects=True),
    )(walker_m, vertex_times, vertex_labels, freq_index, q_index)


def solution(mesh):
    return jax.shard_map(
        local,
        mesh=mesh,
        in_specs=(
            P("walk", "blk", None, None),
            P("walk", "blk", None),
            P("walk", "blk", None),
            P(),
            P("blk"),
        ),
        out_specs=P("blk", None, "walk", None),
        check_vma=False,
    )
```

```python
import functools
import math

import jax
import jax.numpy as jnp
from jax import lax
from jax.experimental import pallas as pl
from jax.experimental.pallas import tpu as pltpu
from jax.sharding import PartitionSpec as P

SIDE = 6
TGRID = 1024
OFFSETS = (0, 1, -1, 2)
SIZES = (2, 3, 3, 2, 2)


def sine(units):
    wrapped = ((units + 1024) & 2047) - 1024
    folded = jnp.where(wrapped > 512, 1024 - wrapped, wrapped)
    folded = jnp.where(wrapped < -512, -1024 - wrapped, folded)
    x = folded.astype(jnp.float32) * (math.pi / 1024.0)
    y = x * x
    total = jnp.full_like(y, 1.0 / math.factorial(13))
    for order in (11, 9, 7, 5, 3, 1):
        sign = -1.0 if (order // 2) % 2 else 1.0
        total = total * y + sign / math.factorial(order)
    return total * x


def sixth_turn(m):
    r = m - 6 * ((m * 10923) >> 16)
    half = jnp.where((r == 1) | (r == 5), 0.5, -0.5)
    cosine = jnp.where(r == 0, 1.0, jnp.where(r == 3, -1.0, half))
    root = math.sqrt(3.0) / 2.0
    side = jnp.where(r < 3, root, -root)
    return cosine.astype(jnp.float32), jnp.where((r == 0) | (r == 3), 0.0, side).astype(jnp.float32)


def visits(groups):
    order = [(0, 0), (0, "p"), (1, 0), (0, "c"), (1, "p")]
    order += [(z, 0) for z in range(2, min(groups, 3))] + [(0, 3)]
    order += [(z, 0) for z in range(3, groups)] + [(1, "c"), (1, 3)]
    order += [(z, "p") for z in range(2, groups)] + [(z, "c") for z in range(2, groups)]
    return order + [(z, 3) for z in range(2, groups)]


def blocks(walkers):
    out = [((1,), "T1 L1 G1".split()), ((2,), "T2 L2".split())]

    def alone(visit, tiles=3):
        last = visit - 1
        return [f"g{last}"] * tiles + [f"T{visit}", f"L{visit}", f"G{last}"]

    out.append(((3,), alone(3, 2)))
    ready, sizes = 4, list(SIZES)
    while ready < walkers:
        size = sizes.pop(0) if sizes else 2
        coming = tuple(range(ready, min(ready + size, walkers)))
        ready += len(coming)
        out.append((coming, [op for visit in coming for op in alone(visit)]))
    out.append(((), [f"G{walkers - 1}"]))
    return out


def across(w, z, groups):
    if groups & (groups - 1):
        return lax.rem(w + groups - z, groups)
    bit, there = 1, w
    while bit < groups:
        if z & bit:
            there = there + bit - 2 * bit * lax.rem(w // bit, 2)
        bit *= 2
    return there


def kernel(
    groups, owners, m_in, t_in, l_in, freq_ref, q_ref, out_ref,
    pack_ref, send_sem, recv_sem, relay_sem, odd, *stages,
):
    walkers = groups * len(OFFSETS)
    order = [(z, d) for z in range(groups) for d in range(len(OFFSETS))]
    w = lax.axis_index("walk")
    b = lax.axis_index("blk")
    v = m_in.shape[-1]
    nf = freq_ref.shape[0]
    own = out_ref.shape[2]
    cols = out_ref.shape[3]
    tables = [stages[3 * i : 3 * i + 3] for i in range(3)]
    lefts = [stages[9 + 2 * i : 11 + 2 * i] for i in range(2)]

    def place(z, d):
        where = {"blk": lax.rem(b + owners - OFFSETS[d], owners)} if d else {}
        return where | ({"walk": across(w, z, groups)} if z else {})

    turned = lax.rem(b, 2)
    beside = {"blk": b + 1 - 2 * turned}

    def copy(source, slot, device, sent=None):
        return pltpu.make_async_remote_copy(
            src_ref=pack_ref.at[source],
            dst_ref=pack_ref.at[slot],
            send_sem=send_sem.at[slot] if sent is None else relay_sem.at[sent],
            recv_sem=recv_sem.at[slot],
            device_id=device,
            device_id_type=pl.DeviceIdType.MESH,
        )

    def arrived(slot):
        copy(0, slot, place(1, 0)).wait_recv()

    def relay(z):
        return copy(order.index((z, 1)), order.index((z, 3)), beside, z)

    def spread(z):
        here = order.index((z, 0))
        for d in (1, 2):
            copy(here, order.index((z, d)), place(0, d)).start()

        @pl.when(turned == 1)
        def _():
            copy(here, order.index((z, 3)), place(0, 3)).start()

    barrier = pltpu.get_barrier_semaphore()
    peers = [{"walk": lax.rem(w + z, groups)} for z in range(1, groups)]
    reach = sorted({d % owners for d in OFFSETS + tuple(-d for d in OFFSETS)} - {0})
    peers += [{"blk": lax.rem(b + d, owners)} for d in reach]
    for peer in peers:
        pl.semaphore_signal(barrier, inc=1, device_id=peer, device_id_type=pl.DeviceIdType.MESH)

    pack_ref[0, 0:v] = m_in[0, 0]
    times = t_in[0]
    line = lax.broadcasted_iota(jnp.int32, (8, v), 0)
    notes = jnp.where(line == 0, times >> 5, jnp.where(line == 1, times & 31, l_in[0]))
    pack_ref[0, v : v + 8] = notes.astype(jnp.float32).astype(jnp.bfloat16)

    window = own if own % 16 == 0 else (own + 23) // 16 * 16
    first = w * own
    spare = lax.rem(first, 16)
    start = pl.multiple_of(first - spare, 16)

    row = lax.broadcasted_iota(jnp.int32, (nf, v), 0)
    freq = jnp.zeros((nf, v), jnp.int32)
    for f in range(nf):
        freq = jnp.where(row == f, 2 * freq_ref[f] + 1, freq)
    odd[...] = freq
    q = q_ref[0]
    qx = (q * 43) >> 8
    qy = q - SIDE * qx

    scale = 1.0 / (v * v * walkers)
    half = SIDE // 2
    low, high = slice(0, v), slice(v, 2 * v)
    contract = (((1,), (1,)), ((), ()))

    for plain, _, _ in tables:
        plain[...] = jnp.zeros_like(plain)
    def tabulate(visit):
        slot = held(visit)
        plain, turned_m, table = tables[visit % len(tables)]
        notes = pack_ref[slot, v : v + 8].astype(jnp.float32).astype(jnp.int32)
        times = (notes[0:1] << 5) + notes[1:2]
        labels = notes[2:3]
        sx = (labels * 43) >> 8
        sy = labels - SIDE * sx

        matrix = pack_ref[slot, 0:v]
        plain[low, low] = matrix
        plain[high, high] = matrix
        cu, su = sixth_turn(qx * sx + qy * sy)
        cu = jnp.broadcast_to(cu, (v, v))
        su = jnp.broadcast_to(su, (v, v))
        ct, st = cu.T, su.T
        wide = matrix.astype(jnp.float32) * scale
        re = (wide * (ct * cu + st * su)).astype(jnp.bfloat16)
        im = (wide * (ct * su - st * cu)).astype(jnp.bfloat16)
        turned_m[low, low] = re
        turned_m[high, high] = re
        turned_m[low, high] = im
        turned_m[high, low] = -im

        units = (odd[...] * times) & 2047
        cx, ox = sixth_turn(sx)
        cy, oy = sixth_turn(sy)
        flip_x = (1 - 2 * (sx & 1)).astype(jnp.float32).astype(jnp.bfloat16)
        flip_y = (1 - 2 * (sy & 1)).astype(jnp.float32)
        c, s = sine(units + 512), sine(units)
        for kx in range(half):
            line = [(c, s)]
            for ky in range(1, half):
                c1, s1 = line[-1]
                line.append((c1 * cy + s1 * oy, s1 * cy - c1 * oy))
            line += [(c1 * flip_y, s1 * flip_y) for c1, s1 in line]
            for pair in range(half):
                rows = slice(nf * (SIDE * kx + 2 * pair), nf * (SIDE * kx + 2 * pair + 2))
                far = slice(rows.start + nf * SIDE * half, rows.stop + nf * SIDE * half)
                for side, lanes in enumerate((low, high)):
                    both = jnp.concatenate(
                        [line[2 * pair][side], line[2 * pair + 1][side]], axis=0
                    ).astype(jnp.bfloat16)
                    table[rows, lanes] = both
                    table[far, lanes] = both * flip_x
            c, s = c * cx + s * ox, s * cx - c * ox

    def lift(visit):
        plain, turned_m, table = tables[visit % len(tables)]
        left_s, left_f = lefts[visit % len(lefts)]
        mine = table[pl.ds(start, window), :]
        for ref, wide in (
            (left_s, jnp.dot(mine, turned_m[...], preferred_element_type=jnp.float32)),
            (left_f, lax.dot_general(mine, plain[...], contract, preferred_element_type=jnp.float32)),
        ):
            if window > own:
                wide = jnp.where(spare > 0, wide[8 : 8 + own], wide[:own])
            for tile in range(own // 8):
                part = wide[8 * tile : 8 * tile + 8]
                re, im = part[:, low], part[:, high]
                rows = slice(16 * tile, 16 * tile + 16)
                ref[rows, low] = jnp.concatenate([re, im], axis=0).astype(jnp.bfloat16)
                ref[rows, high] = jnp.concatenate([im, -re], axis=0).astype(jnp.bfloat16)

    def gather_terms(visit):
        table = tables[visit % len(tables)][2]
        left_s, left_f = lefts[visit % len(lefts)]
        begun = visit > 0

        def add(ref, place, term):
            if begun:
                ref[place] += term
            else:
                ref[place] = term

        for begin in range(0, cols, 256):
            end = min(begin + 256, cols)
            shifted = lax.dot_general(
                left_s[...], table[begin:end], contract, preferred_element_type=jnp.float32
            )
            flipped = lax.dot_general(
                left_f[...], table[begin:end], contract, preferred_element_type=jnp.float32
            )
            for tile in range(own // 8):
                re, im = slice(16 * tile, 16 * tile + 8), slice(16 * tile + 8, 16 * tile + 16)
                rows = slice(8 * tile, 8 * tile + 8)
                sr, si, fr, fi = shifted[re], shifted[im], flipped[re], flipped[im]
                add(out_ref, (0, 0, rows, slice(begin, end)), sr * fr + si * fi)
                add(out_ref, (0, 1, rows, slice(begin, end)), si * fr - sr * fi)
            yield

    def held(visit):
        z, d = plan[visit]
        d = {"p": 1 + turned, "c": 2 - turned}.get(d, d)
        return z * len(OFFSETS) + d

    def await_visits(coming):
        for visit in coming:
            arrived(held(visit))
            z, d = plan[visit]
            if z and not d:
                spread(z)
            if d == "c":
                @pl.when(turned == 1)
                def _(z=z):
                    relay(z).start()

    plan = visits(groups)
    gathers = {}

    def run(ops):
        for op in ops:
            kind, visit = op[0], int(op[1:])
            if kind == "T":
                tabulate(visit)
            elif kind == "L":
                lift(visit)
            else:
                gathers.setdefault(visit, gather_terms(visit))
                for _ in gathers[visit]:
                    if kind == "g":
                        break

    pl.semaphore_wait(barrier, len(peers))
    for z in range(1, groups):
        if z == 2:
            spread(0)
        copy(0, order.index((z, 0)), place(z, 0)).start()
    if groups == 2:
        spread(0)
    run(("T0", "L0", "G0"))
    for coming, ops in blocks(walkers):
        await_visits(coming)
        run(ops)
    for slot, (z, d) in enumerate(order):
        if slot and d != 3:
            copy(0, slot, place(1, 0)).wait_send()

    @pl.when(turned == 1)
    def _():
        for z in range(groups):
            copy(0, order.index((z, 3)), place(1, 0)).wait_send()
            relay(z).wait_send()


def local(walker_m, vertex_times, vertex_labels, freq_index, q_index):
    groups = lax.axis_size("walk")
    owners = lax.axis_size("blk")
    v = walker_m.shape[-1]
    nf = freq_index.shape[0]
    k = SIDE * SIDE * nf
    own = k // groups
    walkers = groups * len(OFFSETS)
    window = own if own % 16 == 0 else (own + 23) // 16 * 16
    held = max(k, max(own * w // 16 * 16 + window for w in range(groups)))
    vmem = pl.BlockSpec(memory_space=pltpu.VMEM)
    smem = pl.BlockSpec(memory_space=pltpu.SMEM)
    bf16 = jnp.bfloat16
    table = [
        pltpu.VMEM((2 * v, 2 * v), bf16),
        pltpu.VMEM((2 * v, 2 * v), bf16),
        pltpu.VMEM((held, 2 * v), bf16),
    ]
    left = [
        pltpu.VMEM((2 * own, 2 * v), bf16),
        pltpu.VMEM((2 * own, 2 * v), bf16),
    ]
    return pl.pallas_call(
        functools.partial(kernel, groups, owners),
        out_shape=pltpu.VMEM((1, 2, own, k), jnp.float32),
        in_specs=[vmem, vmem, vmem, smem, smem],
        out_specs=vmem,
        scratch_shapes=[
            pltpu.VMEM((walkers, v + 8, v), bf16),
            pltpu.SemaphoreType.DMA((walkers,)),
            pltpu.SemaphoreType.DMA((walkers,)),
            pltpu.SemaphoreType.DMA((groups,)),
            pltpu.VMEM((nf, v), jnp.int32),
            *table * 3,
            *left * 2,
        ],
        compiler_params=pltpu.CompilerParams(
            collective_id=0,
            has_side_effects=True,
        ),
    )(walker_m, vertex_times, vertex_labels, freq_index, q_index)


def solution(mesh):
    return jax.shard_map(
        local,
        mesh=mesh,
        in_specs=(
            P("walk", "blk", None, None),
            P("walk", "blk", None),
            P("walk", "blk", None),
            P(),
            P("blk"),
        ),
        out_specs=P("blk", None, "walk", None),
        check_vma=False,
    )
```

```python
import functools
import math

import jax
import jax.numpy as jnp
from jax import lax
from jax.experimental import pallas as pl
from jax.experimental.pallas import tpu as pltpu
from jax.sharding import PartitionSpec as P

SIDE = 6
TGRID = 1024
OFFSETS = (0, 1, -1, 2)
SIZES = (2, 3, 4, 2, 1)


def sine(units):
    wrapped = ((units + 1024) & 2047) - 1024
    folded = jnp.where(wrapped > 512, 1024 - wrapped, wrapped)
    folded = jnp.where(wrapped < -512, -1024 - wrapped, folded)
    x = folded.astype(jnp.float32) * (math.pi / 1024.0)
    y = x * x
    total = jnp.full_like(y, 1.0 / math.factorial(13))
    for order in (11, 9, 7, 5, 3, 1):
        sign = -1.0 if (order // 2) % 2 else 1.0
        total = total * y + sign / math.factorial(order)
    return total * x


def sixth_turn(m):
    r = m - 6 * ((m * 10923) >> 16)
    half = jnp.where((r == 1) | (r == 5), 0.5, -0.5)
    cosine = jnp.where(r == 0, 1.0, jnp.where(r == 3, -1.0, half))
    root = math.sqrt(3.0) / 2.0
    side = jnp.where(r < 3, root, -root)
    return cosine.astype(jnp.float32), jnp.where((r == 0) | (r == 3), 0.0, side).astype(jnp.float32)


def visits(groups):
    order = [(0, 0), (0, "p"), (1, 0), (0, "c")]
    order += [(z, 0) for z in range(2, min(groups, 3))] + [(1, "p")]
    order += [(z, 0) for z in range(3, groups)] + [(0, 3), (1, "c")]
    order += [(z, "p") for z in range(2, min(groups, 3))] + [(1, 3)]
    order += [(z, "c") for z in range(2, min(groups, 3))]
    order += [(z, d) for d in ("p", "c") for z in range(3, groups)]
    return order + [(z, 3) for z in range(2, groups)]


def blocks(walkers):
    out = [((1,), "T1 L1 G1".split()), ((2,), "T2 L2".split())]

    def alone(visit, tiles=3):
        last = visit - 1
        return [f"g{last}"] * tiles + [f"T{visit}", f"L{visit}", f"G{last}"]

    out.append(((3,), alone(3, 2)))
    ready, sizes = 4, list(SIZES)
    while ready < walkers:
        size = sizes.pop(0) if sizes else 2
        coming = tuple(range(ready, min(ready + size, walkers)))
        ready += len(coming)
        out.append((coming, [op for visit in coming for op in alone(visit)]))
    out.append(((), [f"G{walkers - 1}"]))
    return out


def across(w, z, groups):
    if groups & (groups - 1):
        return lax.rem(w + groups - z, groups)
    bit, there = 1, w
    while bit < groups:
        if z & bit:
            there = there + bit - 2 * bit * lax.rem(w // bit, 2)
        bit *= 2
    return there


def kernel(
    groups, owners, m_in, t_in, l_in, freq_ref, q_ref, out_ref,
    pack_ref, send_sem, recv_sem, relay_sem, odd, *stages,
):
    walkers = groups * len(OFFSETS)
    order = [(z, d) for z in range(groups) for d in range(len(OFFSETS))]
    w = lax.axis_index("walk")
    b = lax.axis_index("blk")
    v = m_in.shape[-1]
    nf = freq_ref.shape[0]
    own = out_ref.shape[2]
    cols = out_ref.shape[3]
    tables = [stages[3 * i : 3 * i + 3] for i in range(3)]
    lefts = [stages[9 + 2 * i : 11 + 2 * i] for i in range(2)]

    def place(z, d):
        where = {"blk": lax.rem(b + owners - OFFSETS[d], owners)} if d else {}
        return where | ({"walk": across(w, z, groups)} if z else {})

    turned = lax.rem(b, 2)
    beside = {"blk": b + 1 - 2 * turned}

    def copy(source, slot, device, sent=None):
        return pltpu.make_async_remote_copy(
            src_ref=pack_ref.at[source],
            dst_ref=pack_ref.at[slot],
            send_sem=send_sem.at[slot] if sent is None else relay_sem.at[sent],
            recv_sem=recv_sem.at[slot],
            device_id=device,
            device_id_type=pl.DeviceIdType.MESH,
        )

    def arrived(slot):
        copy(0, slot, place(1, 0)).wait_recv()

    def relay(z):
        return copy(order.index((z, 1)), order.index((z, 3)), beside, z)

    def spread(z):
        here = order.index((z, 0))
        for d in (1, 2):
            copy(here, order.index((z, d)), place(0, d)).start()

        @pl.when(turned == 1)
        def _():
            copy(here, order.index((z, 3)), place(0, 3)).start()

    barrier = pltpu.get_barrier_semaphore()
    peers = [{"walk": lax.rem(w + z, groups)} for z in range(1, groups)]
    reach = sorted({d % owners for d in OFFSETS + tuple(-d for d in OFFSETS)} - {0})
    peers += [{"blk": lax.rem(b + d, owners)} for d in reach]
    for peer in peers:
        pl.semaphore_signal(barrier, inc=1, device_id=peer, device_id_type=pl.DeviceIdType.MESH)

    pack_ref[0, 0:v] = m_in[0, 0]
    times = t_in[0]
    line = lax.broadcasted_iota(jnp.int32, (8, v), 0)
    notes = jnp.where(line == 0, times >> 5, jnp.where(line == 1, times & 31, l_in[0]))
    pack_ref[0, v : v + 8] = notes.astype(jnp.float32).astype(jnp.bfloat16)

    window = own if own % 16 == 0 else (own + 23) // 16 * 16
    first = w * own
    spare = lax.rem(first, 16)
    start = pl.multiple_of(first - spare, 16)

    row = lax.broadcasted_iota(jnp.int32, (nf, v), 0)
    freq = jnp.zeros((nf, v), jnp.int32)
    for f in range(nf):
        freq = jnp.where(row == f, 2 * freq_ref[f] + 1, freq)
    odd[...] = freq
    q = q_ref[0]
    qx = (q * 43) >> 8
    qy = q - SIDE * qx

    scale = 1.0 / (v * v * walkers)
    half = SIDE // 2
    low, high = slice(0, v), slice(v, 2 * v)
    contract = (((1,), (1,)), ((), ()))

    for plain, _, _ in tables:
        plain[...] = jnp.zeros_like(plain)
    def tabulate(visit):
        slot = held(visit)
        plain, turned_m, table = tables[visit % len(tables)]
        notes = pack_ref[slot, v : v + 8].astype(jnp.float32).astype(jnp.int32)
        times = (notes[0:1] << 5) + notes[1:2]
        labels = notes[2:3]
        sx = (labels * 43) >> 8
        sy = labels - SIDE * sx

        matrix = pack_ref[slot, 0:v]
        plain[low, low] = matrix
        plain[high, high] = matrix
        cu, su = sixth_turn(qx * sx + qy * sy)
        cu = jnp.broadcast_to(cu, (v, v))
        su = jnp.broadcast_to(su, (v, v))
        ct, st = cu.T, su.T
        wide = matrix.astype(jnp.float32) * scale
        re = (wide * (ct * cu + st * su)).astype(jnp.bfloat16)
        im = (wide * (ct * su - st * cu)).astype(jnp.bfloat16)
        turned_m[low, low] = re
        turned_m[high, high] = re
        turned_m[low, high] = im
        turned_m[high, low] = -im

        units = (odd[...] * times) & 2047
        cx, ox = sixth_turn(sx)
        cy, oy = sixth_turn(sy)
        flip_x = (1 - 2 * (sx & 1)).astype(jnp.float32).astype(jnp.bfloat16)
        flip_y = (1 - 2 * (sy & 1)).astype(jnp.float32)
        c, s = sine(units + 512), sine(units)
        for kx in range(half):
            line = [(c, s)]
            for ky in range(1, half):
                c1, s1 = line[-1]
                line.append((c1 * cy + s1 * oy, s1 * cy - c1 * oy))
            line += [(c1 * flip_y, s1 * flip_y) for c1, s1 in line]
            for pair in range(half):
                rows = slice(nf * (SIDE * kx + 2 * pair), nf * (SIDE * kx + 2 * pair + 2))
                far = slice(rows.start + nf * SIDE * half, rows.stop + nf * SIDE * half)
                for side, lanes in enumerate((low, high)):
                    both = jnp.concatenate(
                        [line[2 * pair][side], line[2 * pair + 1][side]], axis=0
                    ).astype(jnp.bfloat16)
                    table[rows, lanes] = both
                    table[far, lanes] = both * flip_x
            c, s = c * cx + s * ox, s * cx - c * ox

    def lift(visit):
        plain, turned_m, table = tables[visit % len(tables)]
        left_s, left_f = lefts[visit % len(lefts)]
        mine = table[pl.ds(start, window), :]
        for ref, wide in (
            (left_s, jnp.dot(mine, turned_m[...], preferred_element_type=jnp.float32)),
            (left_f, lax.dot_general(mine, plain[...], contract, preferred_element_type=jnp.float32)),
        ):
            if window > own:
                wide = jnp.where(spare > 0, wide[8 : 8 + own], wide[:own])
            for tile in range(own // 8):
                part = wide[8 * tile : 8 * tile + 8]
                re, im = part[:, low], part[:, high]
                rows = slice(16 * tile, 16 * tile + 16)
                ref[rows, low] = jnp.concatenate([re, im], axis=0).astype(jnp.bfloat16)
                ref[rows, high] = jnp.concatenate([im, -re], axis=0).astype(jnp.bfloat16)

    def gather_terms(visit):
        table = tables[visit % len(tables)][2]
        left_s, left_f = lefts[visit % len(lefts)]
        begun = visit > 0

        def add(ref, place, term):
            if begun:
                ref[place] += term
            else:
                ref[place] = term

        for begin in range(0, cols, 256):
            end = min(begin + 256, cols)
            shifted = lax.dot_general(
                left_s[...], table[begin:end], contract, preferred_element_type=jnp.float32
            )
            flipped = lax.dot_general(
                left_f[...], table[begin:end], contract, preferred_element_type=jnp.float32
            )
            for tile in range(own // 8):
                re, im = slice(16 * tile, 16 * tile + 8), slice(16 * tile + 8, 16 * tile + 16)
                rows = slice(8 * tile, 8 * tile + 8)
                sr, si, fr, fi = shifted[re], shifted[im], flipped[re], flipped[im]
                add(out_ref, (0, 0, rows, slice(begin, end)), sr * fr + si * fi)
                add(out_ref, (0, 1, rows, slice(begin, end)), si * fr - sr * fi)
            yield

    def held(visit):
        z, d = plan[visit]
        d = {"p": 1 + turned, "c": 2 - turned}.get(d, d)
        return z * len(OFFSETS) + d

    def await_visits(coming):
        for visit in coming:
            arrived(held(visit))
            z, d = plan[visit]
            if z and not d:
                spread(z)
            if d == "c":
                @pl.when(turned == 1)
                def _(z=z):
                    relay(z).start()

    plan = visits(groups)
    gathers = {}

    def run(ops):
        for op in ops:
            kind, visit = op[0], int(op[1:])
            if kind == "T":
                tabulate(visit)
            elif kind == "L":
                lift(visit)
            else:
                gathers.setdefault(visit, gather_terms(visit))
                for _ in gathers[visit]:
                    if kind == "g":
                        break

    pl.semaphore_wait(barrier, len(peers))
    for z in range(1, groups):
        if z == 2:
            spread(0)
        copy(0, order.index((z, 0)), place(z, 0)).start()
    if groups == 2:
        spread(0)
    run(("T0", "L0", "G0"))
    for coming, ops in blocks(walkers):
        await_visits(coming)
        run(ops)
    for slot, (z, d) in enumerate(order):
        if slot and d != 3:
            copy(0, slot, place(1, 0)).wait_send()

    @pl.when(turned == 1)
    def _():
        for z in range(groups):
            copy(0, order.index((z, 3)), place(1, 0)).wait_send()
            relay(z).wait_send()


def local(walker_m, vertex_times, vertex_labels, freq_index, q_index):
    groups = lax.axis_size("walk")
    owners = lax.axis_size("blk")
    v = walker_m.shape[-1]
    nf = freq_index.shape[0]
    k = SIDE * SIDE * nf
    own = k // groups
    walkers = groups * len(OFFSETS)
    window = own if own % 16 == 0 else (own + 23) // 16 * 16
    held = max(k, max(own * w // 16 * 16 + window for w in range(groups)))
    vmem = pl.BlockSpec(memory_space=pltpu.VMEM)
    smem = pl.BlockSpec(memory_space=pltpu.SMEM)
    bf16 = jnp.bfloat16
    table = [
        pltpu.VMEM((2 * v, 2 * v), bf16),
        pltpu.VMEM((2 * v, 2 * v), bf16),
        pltpu.VMEM((held, 2 * v), bf16),
    ]
    left = [
        pltpu.VMEM((2 * own, 2 * v), bf16),
        pltpu.VMEM((2 * own, 2 * v), bf16),
    ]
    return pl.pallas_call(
        functools.partial(kernel, groups, owners),
        out_shape=pltpu.VMEM((1, 2, own, k), jnp.float32),
        in_specs=[vmem, vmem, vmem, smem, smem],
        out_specs=vmem,
        scratch_shapes=[
            pltpu.VMEM((walkers, v + 8, v), bf16),
            pltpu.SemaphoreType.DMA((walkers,)),
            pltpu.SemaphoreType.DMA((walkers,)),
            pltpu.SemaphoreType.DMA((groups,)),
            pltpu.VMEM((nf, v), jnp.int32),
            *table * 3,
            *left * 2,
        ],
        compiler_params=pltpu.CompilerParams(
            collective_id=0,
            has_side_effects=True,
        ),
    )(walker_m, vertex_times, vertex_labels, freq_index, q_index)


def solution(mesh):
    return jax.shard_map(
        local,
        mesh=mesh,
        in_specs=(
            P("walk", "blk", None, None),
            P("walk", "blk", None),
            P("walk", "blk", None),
            P(),
            P("blk"),
        ),
        out_specs=P("blk", None, "walk", None),
        check_vma=False,
    )
```

```python
import functools
import math

import jax
import jax.numpy as jnp
from jax import lax
from jax.experimental import pallas as pl
from jax.experimental.pallas import tpu as pltpu
from jax.sharding import PartitionSpec as P

SIDE = 6
TGRID = 1024
OFFSETS = (0, 1, -1, 2)
SIZES = (2, 3, 4, 2, 1)


def sine(units):
    wrapped = ((units + 1024) & 2047) - 1024
    folded = jnp.where(wrapped > 512, 1024 - wrapped, wrapped)
    folded = jnp.where(wrapped < -512, -1024 - wrapped, folded)
    x = folded.astype(jnp.float32) * (math.pi / 1024.0)
    y = x * x
    total = jnp.full_like(y, 1.0 / math.factorial(13))
    for order in (11, 9, 7, 5, 3, 1):
        sign = -1.0 if (order // 2) % 2 else 1.0
        total = total * y + sign / math.factorial(order)
    return total * x


def sixth_turn(m):
    r = m - 6 * ((m * 10923) >> 16)
    half = jnp.where((r == 1) | (r == 5), 0.5, -0.5)
    cosine = jnp.where(r == 0, 1.0, jnp.where(r == 3, -1.0, half))
    root = math.sqrt(3.0) / 2.0
    side = jnp.where(r < 3, root, -root)
    return cosine.astype(jnp.float32), jnp.where((r == 0) | (r == 3), 0.0, side).astype(jnp.float32)


def visits(groups):
    order = [(0, 0), (0, "p"), (1, 0), (0, "c")]
    order += [(z, 0) for z in range(2, min(groups, 3))] + [(1, "p")]
    order += [(z, 0) for z in range(3, groups)] + [(0, 3), (1, "c")]
    order += [(z, "p") for z in range(2, min(groups, 3))] + [(1, 3)]
    order += [(z, "c") for z in range(2, min(groups, 3))]
    order += [(z, d) for d in ("p", "c") for z in range(3, groups)]
    return order + [(z, 3) for z in range(2, groups)]


def blocks(walkers):
    out = [((1,), "T1 L1 G1".split()), ((2,), "T2 L2".split())]

    def alone(visit, tiles=3):
        last = visit - 1
        return [f"g{last}"] * tiles + [f"T{visit}", f"L{visit}", f"G{last}"]

    out.append(((3,), alone(3, 2)))
    ready, sizes = 4, list(SIZES)
    while ready < walkers:
        size = sizes.pop(0) if sizes else 2
        coming = tuple(range(ready, min(ready + size, walkers)))
        ready += len(coming)
        out.append((coming, [op for visit in coming for op in alone(visit)]))
    out.append(((), [f"G{walkers - 1}"]))
    return out


def across(w, z, groups):
    if groups & (groups - 1):
        return lax.rem(w + groups - z, groups)
    bit, there = 1, w
    while bit < groups:
        if z & bit:
            there = there + bit - 2 * bit * lax.rem(w // bit, 2)
        bit *= 2
    return there


def kernel(
    groups, owners, m_in, t_in, l_in, freq_ref, q_ref, out_ref,
    pack_ref, send_sem, recv_sem, relay_sem, odd, *stages,
):
    walkers = groups * len(OFFSETS)
    order = [(z, d) for z in range(groups) for d in range(len(OFFSETS))]
    w = lax.axis_index("walk")
    b = lax.axis_index("blk")
    v = m_in.shape[-1]
    nf = freq_ref.shape[0]
    own = out_ref.shape[2]
    cols = out_ref.shape[3]
    tables = [stages[3 * i : 3 * i + 3] for i in range(3)]
    lefts = [stages[9 + 2 * i : 11 + 2 * i] for i in range(2)]

    def place(z, d):
        where = {"blk": lax.rem(b + owners - OFFSETS[d], owners)} if d else {}
        return where | ({"walk": across(w, z, groups)} if z else {})

    turned = lax.rem(b, 2)
    beside = {"blk": b + 1 - 2 * turned}

    def copy(source, slot, device, sent=None):
        return pltpu.make_async_remote_copy(
            src_ref=pack_ref.at[source],
            dst_ref=pack_ref.at[slot],
            send_sem=send_sem.at[slot] if sent is None else relay_sem.at[sent],
            recv_sem=recv_sem.at[slot],
            device_id=device,
            device_id_type=pl.DeviceIdType.MESH,
        )

    def arrived(slot):
        copy(0, slot, place(1, 0)).wait_recv()

    def relay(z):
        return copy(order.index((z, 1)), order.index((z, 3)), beside, z)

    def spread(z):
        here = order.index((z, 0))
        for d in (1, 2):
            copy(here, order.index((z, d)), place(0, d)).start()

        @pl.when(turned == 1)
        def _():
            copy(here, order.index((z, 3)), place(0, 3)).start()

    barrier = pltpu.get_barrier_semaphore()
    peers = [{"walk": lax.rem(w + z, groups)} for z in range(1, groups)]
    reach = sorted({d % owners for d in OFFSETS + tuple(-d for d in OFFSETS)} - {0})
    peers += [{"blk": lax.rem(b + d, owners)} for d in reach]
    for peer in peers:
        pl.semaphore_signal(barrier, inc=1, device_id=peer, device_id_type=pl.DeviceIdType.MESH)

    pack_ref[0, 0:v] = m_in[0, 0]
    times = t_in[0]
    line = lax.broadcasted_iota(jnp.int32, (8, v), 0)
    notes = jnp.where(line == 0, times >> 5, jnp.where(line == 1, times & 31, l_in[0]))
    pack_ref[0, v : v + 8] = notes.astype(jnp.float32).astype(jnp.bfloat16)

    window = own if own % 16 == 0 else (own + 23) // 16 * 16
    first = w * own
    spare = lax.rem(first, 16)
    start = pl.multiple_of(first - spare, 16)

    row = lax.broadcasted_iota(jnp.int32, (nf, v), 0)
    freq = jnp.zeros((nf, v), jnp.int32)
    for f in range(nf):
        freq = jnp.where(row == f, 2 * freq_ref[f] + 1, freq)
    odd[...] = freq
    q = q_ref[0]
    qx = (q * 43) >> 8
    qy = q - SIDE * qx

    scale = 1.0 / (v * v * walkers)
    half = SIDE // 2
    low, high = slice(0, v), slice(v, 2 * v)
    contract = (((1,), (1,)), ((), ()))

    for plain, _, _ in tables:
        plain[...] = jnp.zeros_like(plain)
    def tabulate(visit):
        slot = held(visit)
        plain, turned_m, table = tables[visit % len(tables)]
        notes = pack_ref[slot, v : v + 8].astype(jnp.float32).astype(jnp.int32)
        times = (notes[0:1] << 5) + notes[1:2]
        labels = notes[2:3]
        sx = (labels * 43) >> 8
        sy = labels - SIDE * sx

        matrix = pack_ref[slot, 0:v]
        plain[low, low] = matrix
        plain[high, high] = matrix
        cu, su = sixth_turn(qx * sx + qy * sy)
        cu = jnp.broadcast_to(cu, (v, v))
        su = jnp.broadcast_to(su, (v, v))
        ct, st = cu.T, su.T
        wide = matrix.astype(jnp.float32) * scale
        re = (wide * (ct * cu + st * su)).astype(jnp.bfloat16)
        im = (wide * (ct * su - st * cu)).astype(jnp.bfloat16)
        turned_m[low, low] = re
        turned_m[high, high] = re
        turned_m[low, high] = im
        turned_m[high, low] = -im

        units = (odd[...] * times) & 2047
        cx, ox = sixth_turn(sx)
        cy, oy = sixth_turn(sy)
        flip_x = (1 - 2 * (sx & 1)).astype(jnp.float32).astype(jnp.bfloat16)
        flip_y = (1 - 2 * (sy & 1)).astype(jnp.float32)
        c, s = sine(units + 512), sine(units)
        for kx in range(half):
            line = [(c, s)]
            for ky in range(1, half):
                c1, s1 = line[-1]
                line.append((c1 * cy + s1 * oy, s1 * cy - c1 * oy))
            line += [(c1 * flip_y, s1 * flip_y) for c1, s1 in line]
            for pair in range(half):
                rows = slice(nf * (SIDE * kx + 2 * pair), nf * (SIDE * kx + 2 * pair + 2))
                far = slice(rows.start + nf * SIDE * half, rows.stop + nf * SIDE * half)
                for side, lanes in enumerate((low, high)):
                    both = jnp.concatenate(
                        [line[2 * pair][side], line[2 * pair + 1][side]], axis=0
                    ).astype(jnp.bfloat16)
                    table[rows, lanes] = both
                    table[far, lanes] = both * flip_x
            c, s = c * cx + s * ox, s * cx - c * ox

    def lift(visit):
        plain, turned_m, table = tables[visit % len(tables)]
        left_s, left_f = lefts[visit % len(lefts)]
        mine = table[pl.ds(start, window), :]
        for ref, wide in (
            (left_s, jnp.dot(mine, turned_m[...], preferred_element_type=jnp.float32)),
            (left_f, lax.dot_general(mine, plain[...], contract, preferred_element_type=jnp.float32)),
        ):
            if window > own:
                wide = jnp.where(spare > 0, wide[8 : 8 + own], wide[:own])
            for tile in range(own // 8):
                part = wide[8 * tile : 8 * tile + 8]
                re, im = part[:, low], part[:, high]
                rows = slice(16 * tile, 16 * tile + 16)
                ref[rows, low] = jnp.concatenate([re, im], axis=0).astype(jnp.bfloat16)
                ref[rows, high] = jnp.concatenate([im, -re], axis=0).astype(jnp.bfloat16)

    def gather_terms(visit):
        table = tables[visit % len(tables)][2]
        left_s, left_f = lefts[visit % len(lefts)]
        begun = visit > 0

        def add(ref, place, term):
            if begun:
                ref[place] += term
            else:
                ref[place] = term

        for begin in range(0, cols, 256):
            end = min(begin + 256, cols)
            shifted = lax.dot_general(
                left_s[...], table[begin:end], contract, preferred_element_type=jnp.float32
            )
            flipped = lax.dot_general(
                left_f[...], table[begin:end], contract, preferred_element_type=jnp.float32
            )
            for tile in range(own // 8):
                re, im = slice(16 * tile, 16 * tile + 8), slice(16 * tile + 8, 16 * tile + 16)
                rows = slice(8 * tile, 8 * tile + 8)
                sr, si, fr, fi = shifted[re], shifted[im], flipped[re], flipped[im]
                add(out_ref, (0, 0, rows, slice(begin, end)), sr * fr + si * fi)
                add(out_ref, (0, 1, rows, slice(begin, end)), si * fr - sr * fi)
            yield

    def held(visit):
        z, d = plan[visit]
        d = {"p": 1 + turned, "c": 2 - turned}.get(d, d)
        return z * len(OFFSETS) + d

    def await_visits(coming):
        for visit in coming:
            arrived(held(visit))
            z, d = plan[visit]
            if z and not d:
                spread(z)
            if d == "c":
                @pl.when(turned == 1)
                def _(z=z):
                    relay(z).start()

    plan = visits(groups)
    gathers = {}

    def run(ops):
        for op in ops:
            kind, visit = op[0], int(op[1:])
            if kind == "T":
                tabulate(visit)
            elif kind == "L":
                lift(visit)
            else:
                gathers.setdefault(visit, gather_terms(visit))
                for _ in gathers[visit]:
                    if kind == "g":
                        break

    run(("T0", "L0"))
    pl.semaphore_wait(barrier, len(peers))
    for z in range(1, groups):
        if z == 2:
            spread(0)
        copy(0, order.index((z, 0)), place(z, 0)).start()
    if groups == 2:
        spread(0)
    run(("G0",))
    for coming, ops in blocks(walkers):
        await_visits(coming)
        run(ops)
    for slot, (z, d) in enumerate(order):
        if slot and d != 3:
            copy(0, slot, place(1, 0)).wait_send()

    @pl.when(turned == 1)
    def _():
        for z in range(groups):
            copy(0, order.index((z, 3)), place(1, 0)).wait_send()
            relay(z).wait_send()


def local(walker_m, vertex_times, vertex_labels, freq_index, q_index):
    groups = lax.axis_size("walk")
    owners = lax.axis_size("blk")
    v = walker_m.shape[-1]
    nf = freq_index.shape[0]
    k = SIDE * SIDE * nf
    own = k // groups
    walkers = groups * len(OFFSETS)
    window = own if own % 16 == 0 else (own + 23) // 16 * 16
    held = max(k, max(own * w // 16 * 16 + window for w in range(groups)))
    vmem = pl.BlockSpec(memory_space=pltpu.VMEM)
    smem = pl.BlockSpec(memory_space=pltpu.SMEM)
    bf16 = jnp.bfloat16
    table = [
        pltpu.VMEM((2 * v, 2 * v), bf16),
        pltpu.VMEM((2 * v, 2 * v), bf16),
        pltpu.VMEM((held, 2 * v), bf16),
    ]
    left = [
        pltpu.VMEM((2 * own, 2 * v), bf16),
        pltpu.VMEM((2 * own, 2 * v), bf16),
    ]
    return pl.pallas_call(
        functools.partial(kernel, groups, owners),
        out_shape=pltpu.VMEM((1, 2, own, k), jnp.float32),
        in_specs=[vmem, vmem, vmem, smem, smem],
        out_specs=vmem,
        scratch_shapes=[
            pltpu.VMEM((walkers, v + 8, v), bf16),
            pltpu.SemaphoreType.DMA((walkers,)),
            pltpu.SemaphoreType.DMA((walkers,)),
            pltpu.SemaphoreType.DMA((groups,)),
            pltpu.VMEM((nf, v), jnp.int32),
            *table * 3,
            *left * 2,
        ],
        compiler_params=pltpu.CompilerParams(
            collective_id=0,
            has_side_effects=True,
        ),
    )(walker_m, vertex_times, vertex_labels, freq_index, q_index)


def solution(mesh):
    return jax.shard_map(
        local,
        mesh=mesh,
        in_specs=(
            P("walk", "blk", None, None),
            P("walk", "blk", None),
            P("walk", "blk", None),
            P(),
            P("blk"),
        ),
        out_specs=P("blk", None, "walk", None),
        check_vma=False,
    )
```
